512 devices in a mesh: wave: 64 (over z, y), lev: 8 (over x, core).
Axes of the slice: x: 4, y: 8, z: 8, core: 2. Of those that a mesh axis runs over, the one named last changes fastest.
Arguments:
- control: bfloat16 [2, 256, 256, 2, 512], P(None, 'wave', 'lev'), may hold values from -6 to 6
- wave_of_slot: int32 [256], replicated, may hold values from 0 to 255, each once
- legendre: bfloat16 [256, 256, 256], P('wave', 'lev'), may hold values from -0.375 to 0.375
- vertical: bfloat16 [4, 4, 128, 128], replicated, may hold values from -0.5 to 0.5
- points: int32 [256], P('wave'), may hold values from 128 to 512
- lat_band: int32 [256], P('wave'), may hold values from 0 to 7, never falling along the last dimension, each value on 1 to 64 neighbouring positions
- grid_scale: float32 [8, 512], P(None, 'lev'), may hold values from 0.5 to 2
- obs_weight: bfloat16 [256, 512, 512], P('wave', 'lev'), may hold values from 0.19921875 to 1
Outputs:
- increment: bfloat16 [2, 256, 512, 512], P(None, 'wave', 'lev')
- gradient: bfloat16 [2, 256, 256, 2, 512], P(None, 'wave', 'lev')
The draws below stay inside these ranges and needn't reach their ends.
Inputs may be any that keep to these rules, and one draw needn't show every extreme that they name: `wave_of_slot`: each zonal wavenumber 0 to 255 stands in exactly one slot. `lat_band`: band numbers never fall from one latitude to the next, and each band covers 1 to 64 latitudes.
All inputs are finite; a program needn't handle non-finite values.
Results may differ from the reference program's by a relative error of at most 0.007.
Values may be sent and summed in bfloat16 or wider, within the bound.
A program may use at most 64 MiB of HBM per device.

```python
import math
import jax
import jax.numpy as jnp
import numpy as np

WAVES = 256
LATITUDES = 256
LONGITUDES = 512
LEVELS = 128
VARIABLES = 4
COV_BANDS = 4
LAT_BANDS = 8
MEMBERS = 2
COLUMNS = 512


def plant(drawn, own_key, least, top_value):
    index_at = [jax.random.randint(jax.random.fold_in(own_key, axis), (), 0, length) for axis, length in enumerate(drawn.shape)]
    widest = drawn.shape.index(max(drawn.shape))
    next_to = index_at[:widest] + [(index_at[widest] + 1) % drawn.shape[widest]] + index_at[widest + 1:]
    return drawn.at[tuple(index_at)].set(least).at[tuple(next_to)].set(top_value)


def level_of(stream_key, extent, shards, least, high):
    gain, own = 1.0, jax.random.fold_in(stream_key, 6)
    for position, blocks in shards:
        steps = jnp.exp(jax.random.uniform(jax.random.fold_in(own, position), (blocks,), jnp.float32, least / len(shards), high / len(shards)))
        gain = gain * jnp.repeat(steps, extent[position] // blocks).reshape([-1 if axis == position else 1 for axis in range(len(extent))])
    return gain


def length_profile(count, total, most, skew):
    portions = [(1 << 20) // math.isqrt(rank ** skew) + 1 for rank in range(2, count + 1)]
    rest, holding = total - most - (count - 1), [1] * (count - 1)
    while rest > 0:
        candidates = [i for i in range(count - 1) if holding[i] < most]
        whole, remaining = sum([portions[i] for i in candidates]), rest
        for i in candidates:
            more = min(most - holding[i], max(1, remaining * portions[i] // whole), rest)
            holding[i] = holding[i] + more
            rest = rest - more
    return np.array([most] + holding)


def ragged_sizes(rng, count, total, reach, slope):
    if count == 2:
        one = jax.random.randint(rng, (), max(1, total - reach), min(reach, total - 1) + 1)
        return jnp.stack([one, total - one])
    tallies = jnp.asarray(length_profile(count, total, reach, slope), jnp.int32)
    couples = (count - 1) // 2
    donor, receiver = tallies[1:1 + 2 * couples:2], tallies[2:2 + 2 * couples:2]
    slack = jnp.minimum(donor - 1, reach - receiver)
    passed = jax.random.randint(jax.random.fold_in(rng, 1), (couples,), 0, 1 << 20) % (slack + 1)
    tallies = tallies.at[1:1 + 2 * couples:2].set(donor - passed).at[2:2 + 2 * couples:2].set(receiver + passed)
    return tallies[jax.random.permutation(jax.random.fold_in(rng, 2), count)]


def scatter_about(key, dims, spread, most, pieces=(), held_as=jnp.bfloat16):
    drawn = jax.random.normal(key, dims, jnp.float32) * spread
    if len(pieces) > 0:
        drawn = level_of(key, dims, pieces, -0.22, 0.18) * drawn
    return jnp.clip(drawn, min=-most, max=most).astype(held_as)


def setup_inputs(seed: int = 0) -> dict:
    splits = jax.random.split(jax.random.key(seed), 9)
    return {
        "control": scatter_about(splits[0], (MEMBERS, WAVES, WAVES, 2, COLUMNS), 1.0, 6.0, ((1, 64), (2, 8))),
        "wave_of_slot": jax.random.permutation(splits[1], WAVES).astype(jnp.int32),
        "legendre": scatter_about(splits[2], (WAVES, WAVES, LATITUDES), WAVES ** -0.5, 0.375, ((0, 64), (1, 8))),
        "vertical": scatter_about(splits[3], (COV_BANDS, VARIABLES, LEVELS, LEVELS), LEVELS ** -0.5, 0.5),
        "points": plant(jax.random.randint(splits[4], (LATITUDES,), LONGITUDES // 4, LONGITUDES + 1), jax.random.fold_in(splits[4], 1), LONGITUDES // 4, LONGITUDES).astype(jnp.int32),
        "lat_band": jnp.searchsorted(jnp.cumsum(ragged_sizes(splits[5], LAT_BANDS, LATITUDES, 2 * LATITUDES // LAT_BANDS, 1)), jnp.arange(LATITUDES), side="right").astype(jnp.int32),
        "grid_scale": jnp.clip(jnp.exp(math.log(2.0) - 1.3862944 * jax.random.uniform(splits[6], (LAT_BANDS, COLUMNS), jnp.float32) ** level_of(splits[6], (LAT_BANDS, COLUMNS), ((1, 8),), -0.2, 0.2)), 0.5, 2.0),
        "obs_weight": jnp.clip(jnp.exp(math.log(1.0) - 1.6133518 * jax.random.uniform(splits[7], (LATITUDES, COLUMNS, LONGITUDES), jnp.float32) ** level_of(splits[7], (LATITUDES, COLUMNS, LONGITUDES), ((0, 64), (1, 8)), -0.2, 0.2)), 0.19921875, 1.0).astype(jnp.bfloat16),
    }


def fourier_table(wave_ids, lat_points):
    lon_index = jnp.arange(LONGITUDES, dtype=jnp.int32)
    remainder = wave_ids[None, :, None] * lon_index[None, None, :] % lat_points[:, None, None]
    angles = 2.0 * math.pi * remainder.astype(jnp.float32) / lat_points.astype(jnp.float32)[:, None, None]
    factor = jnp.where(wave_ids == 0, 1.0, 2.0).astype(jnp.float32) / math.sqrt(4.0 * WAVES)
    inside = lon_index[None, None, :] < lat_points[:, None, None]
    cosine = jnp.where(inside, factor[None, :, None] * jnp.cos(angles), 0.0)
    sine = jnp.where(inside, -factor[None, :, None] * jnp.sin(angles), 0.0)
    return jnp.stack([cosine, sine], axis=2).astype(jnp.bfloat16)

def vertical_apply(field, vertical, live_rows, band_of, forward):
    shaped = field.astype(jnp.float32).reshape(WAVES, WAVES, 2, VARIABLES, LEVELS)
    matrices = vertical.astype(jnp.float32)
    form = 'skpam,alm->skpal' if forward else 'skpal,alm->skpam'
    summed = jnp.zeros(shaped.shape, jnp.float32)
    for index_band in range(COV_BANDS):
        partial_value = jnp.einsum(form, shaped, matrices[index_band])
        chosen = live_rows & (band_of == index_band)
        summed = summed + jnp.where(chosen[:, :, None, None, None], partial_value, 0.0)
    return summed.reshape(WAVES, WAVES, 2, COLUMNS).astype(jnp.bfloat16)

def reference(control, wave_of_slot, legendre, vertical, points, lat_band, grid_scale, obs_weight):
    row_index = jnp.arange(WAVES, dtype=jnp.int32)
    totals_n = wave_of_slot[:, None] + row_index[None, :]
    live_rows = totals_n <= WAVES - 1
    band_of = jnp.minimum(totals_n * COV_BANDS // WAVES, COV_BANDS - 1)
    fourier = fourier_table(wave_of_slot, points).astype(jnp.float32)
    table32 = legendre.astype(jnp.float32)
    lat_scale = grid_scale[lat_band]
    weight32 = obs_weight.astype(jnp.float32)
    increments = []
    gradients = []
    for member in range(MEMBERS):
        spectral = vertical_apply(control[member], vertical, live_rows, band_of, True)
        flat = spectral.astype(jnp.float32).reshape(WAVES, WAVES, 2 * COLUMNS)
        coeffs = jnp.einsum('skt,skq->stq', table32, flat).astype(jnp.bfloat16)
        coeffs32 = coeffs.astype(jnp.float32).reshape(WAVES, LATITUDES, 2, COLUMNS)
        synthesis = jnp.einsum('tspj,stpc->tcj', fourier, coeffs32)
        increment = (synthesis * lat_scale[:, :, None]).astype(jnp.bfloat16)
        weighted = (increment.astype(jnp.float32) * weight32 * lat_scale[:, :, None]).astype(jnp.bfloat16)
        adjoint_fourier = jnp.einsum('tspj,tcj->tspc', fourier, weighted.astype(jnp.float32)).astype(jnp.bfloat16)
        adjoint_flat = adjoint_fourier.astype(jnp.float32).reshape(LATITUDES, WAVES, 2 * COLUMNS)
        adjoint_coeffs = jnp.einsum('skt,tsq->skq', table32, adjoint_flat).astype(jnp.bfloat16)
        adjoint_coeffs = adjoint_coeffs.reshape(WAVES, WAVES, 2, COLUMNS)
        gradient = vertical_apply(adjoint_coeffs, vertical, live_rows, band_of, False)
        increments.append(increment)
        gradients.append(gradient)
    return (jnp.stack(increments, axis=0), jnp.stack(gradients, axis=0))
```

```python
import functools

import jax
import jax.numpy as jnp
from jax import lax
from jax.experimental import pallas as pl
from jax.experimental.pallas import tpu as pltpu
from jax.sharding import PartitionSpec as P

WAVES = 256
LONGITUDES = 512
COV_BANDS = 4
VARIABLES = 4
MESH = pl.DeviceIdType.MESH
F32 = jnp.float32
BF16 = jnp.bfloat16
FAR_FIRST = (4, 3, 5, 2, 6, 1, 7)
SIN = (6.283185302498671, -41.34170040100665, 81.6051311559332, -76.70301094142194,
       42.02588917305049, -14.899698808670236, 3.237922486217859)
COS = (0.9999999998851921, -19.739208743292323, 64.93938906426658, -85.45665800487392,
       60.24212744331612, -26.404643265364264, 7.800052913395129, -1.453015691570865)


def polynomial(terms, s):
    value = jnp.full(s.shape, terms[-1], F32)
    for term in terms[-2::-1]:
        value = value * s + term
    return value


def dot(a, b, dims=((1,), (0,))):
    return lax.dot_general(a, b, (dims, ((), ())), preferred_element_type=F32)


def kernel(
    waves_s, points_s, band_s, waves_v, ctl_h, leg_h, ver_h, scale_h, obs_h,
    inc_h, grad_h,
    ctl, ver, own_leg, scale, obs, inc, grad,
    mask, mix, send_f, recv_f, leg, leg_t, wcol, table,
    a1, b1y, b1z, c1, xf, a2, b2y, b2z, c2, send_b, recv_b,
    in_sem, out_sem, leg_ss, leg_rs, lev_ss, lev_rs, wave_ss, wave_rs,
):
    wave = lax.axis_index("wave")
    lev = lax.axis_index("lev")
    z = wave // 8
    y = lax.rem(wave, 8)

    ins = [
        pltpu.make_async_copy(src, dst, in_sem.at[i])
        for i, (src, dst) in enumerate(
            ((ctl_h, ctl), (ver_h, ver), (leg_h, own_leg), (scale_h, scale), (obs_h, obs))
        )
    ]
    for copy in ins:
        copy.start()

    barrier = pltpu.get_barrier_semaphore()

    def along(i):
        return (
            (wave, lax.rem(lev + i, 8)),
            (z * 8 + lax.rem(y + i, 8), lev),
            (lax.rem(z + i, 8) * 8 + y, lev),
        )

    for i in FAR_FIRST:
        for who in along(i):
            pl.semaphore_signal(barrier, inc=1, device_id=who, device_id_type=MESH)

    row = lax.broadcasted_iota(jnp.int32, (128, 128), 0)
    slot = row // 32
    total = lev * 32 + lax.rem(row, 32)
    for s in range(4):
        total = total + jnp.where(slot == s, waves_s[wave * 4 + s], 0)
    band = jnp.minimum(total * COV_BANDS // WAVES, COV_BANDS - 1)
    for b in range(COV_BANDS):
        chosen = (total <= WAVES - 1) & (band == b)
        mask[b] = jnp.where(chosen, 1.0, 0.0).astype(BF16)

    ins[1].wait()

    def lay(i, carry):
        zero = jnp.zeros((64, 128), BF16)
        v = ver[i]
        for half in range(2):
            piece = v[half * 64 : half * 64 + 64]
            mix[i, half * 128 : half * 128 + 64, 0:128] = piece
            mix[i, half * 128 : half * 128 + 64, 128:256] = zero
            mix[i, half * 128 + 64 : half * 128 + 128, 0:128] = zero
            mix[i, half * 128 + 64 : half * 128 + 128, 128:256] = piece
        return carry

    lax.fori_loop(0, COV_BANDS * VARIABLES, lay, 0)

    ins[0].wait()
    for a in range(VARIABLES):
        both = [ctl[:, a * 128 : a * 128 + 128], ctl[:, 512 + a * 128 : 640 + a * 128]]
        out = jnp.zeros((256, 256), F32)
        for b in range(COV_BANDS):
            m = jnp.concatenate([mask[b], mask[b]], axis=0)
            x = jnp.concatenate([part * m for part in both], axis=1)
            out = out + dot(x, mix[b * VARIABLES + a], ((1,), (1,)))
        out = out.astype(BF16)
        for half in range(2):
            send_f[2 * a + half] = out[:, half * 128 : half * 128 + 128].reshape(2, 4, 32, 128)

    place = lax.broadcasted_iota(jnp.int32, (256, 128), 0)
    wanted = lax.rem(place, 128) // 2 * 4 + place // 128 * 2 + lax.rem(place, 2)
    lane = lax.broadcasted_iota(jnp.int32, (256, 128), 1)
    found = jnp.zeros((256, 128), F32)
    for i in range(2):
        numbers = waves_v[i : i + 1, :].astype(F32)
        found = found + jnp.where(wanted == lane + i * 128, numbers, 0.0)
    wcol[...] = jnp.broadcast_to(jnp.sum(found, axis=1, keepdims=True), (256, 128))

    for t in range(4):
        count = jnp.full((16, LONGITUDES), points_s[t], jnp.int32).astype(F32)
        inverse = 1.0 / count

        def rows_of_table(i, carry, t=t, count=count, inverse=inverse):
            at = pl.multiple_of(i * 16, 16)
            w = wcol[pl.ds(at, 16), :]
            w = jnp.concatenate([w, w, w, w], axis=1)
            j = lax.broadcasted_iota(jnp.int32, (16, LONGITUDES), 1).astype(F32)
            product = w * j
            turns = jnp.floor(product * inverse + 0.5)
            x = (product - turns * count) * inverse
            s = x * x
            factor = jnp.where(w == 0.0, 1.0, 2.0) * (1.0 / 32.0)
            factor = jnp.where(j < count, factor, 0.0)
            table[t, 0, pl.ds(at, 16), :] = (factor * polynomial(COS, s)).astype(BF16)
            table[t, 1, pl.ds(at, 16), :] = (-factor * (x * polynomial(SIN, s))).astype(BF16)
            return carry

        lax.fori_loop(0, 16, rows_of_table, 0)

    ins[2].wait()
    pl.semaphore_wait(barrier, 21)

    def lev_peer(i):
        return lax.rem(lev + i, 8)

    def remote(src, dst, ss, rs, who):
        pltpu.make_async_remote_copy(
            src, dst, ss, rs, device_id=who, device_id_type=MESH
        ).start()

    def arrived(buffer, sem):
        pltpu.make_async_copy(buffer, buffer, sem).wait()

    def send_leg(h):
        for i in FAR_FIRST:
            remote(
                own_leg.at[pl.ds(2 * h, 2)], leg.at[pl.ds(2 * h, 2), lev],
                leg_ss.at[h], leg_rs.at[h], (wave, lev_peer(i)),
            )

    def send_spec(e, h):
        for i in FAR_FIRST:
            v = lev_peer(i)
            remote(
                send_f.at[v, e, pl.ds(2 * h, 2)], recv_f.at[e, pl.ds(2 * h, 2), lev],
                lev_ss.at[0, e, h], lev_rs.at[0, e, h], (wave, v),
            )

    send_leg(0)
    send_spec(0, 0)
    send_leg(1)
    send_spec(0, 1)
    send_spec(1, 0)
    send_spec(1, 1)
    for s in range(4):
        leg[s, lev] = own_leg[s]
        for e in range(2):
            recv_f[e, s, lev] = send_f[lev, e, s]

    sub = lax.broadcasted_iota(jnp.int32, (32, 8, 128), 1)

    def interleave(p, q):
        return (
            jnp.where(sub < 4, p, pltpu.roll(q, 4, 1)),
            jnp.where(sub < 4, pltpu.roll(p, 4, 1), q),
        )

    def first_hop(d, e, h, src, by, bz):
        for i in FAR_FIRST:
            if h == 0:
                k = lax.rem(y + i, 8)
                remote(
                    src.at[e, 0, :, k], by.at[e, y],
                    wave_ss.at[d, 0, e, h], wave_rs.at[d, 0, e, h], (z * 8 + k, lev),
                )
            else:
                k = lax.rem(z + i, 8)
                remote(
                    src.at[e, 1, k], bz.at[e, z],
                    wave_ss.at[d, 0, e, h], wave_rs.at[d, 0, e, h], (k * 8 + y, lev),
                )
        if h == 0:
            by[e, y] = src[e, 0, :, y]
        else:
            bz[e, z] = src[e, 1, z]

    def second_hop(d, e, h, by, bz, dst):
        if h == 0:
            arrived(by.at[e, pl.ds(0, 7)], wave_rs.at[d, 0, e, h])
        else:
            arrived(bz.at[e, pl.ds(0, 7)], wave_rs.at[d, 0, e, h])
        for i in FAR_FIRST:
            if h == 0:
                k = lax.rem(z + i, 8)
                remote(
                    by.at[e, :, k], dst.at[e, 0, z],
                    wave_ss.at[d, 1, e, h], wave_rs.at[d, 1, e, h], (k * 8 + y, lev),
                )
            else:
                k = lax.rem(y + i, 8)
                remote(
                    bz.at[e, :, k], dst.at[e, 1, :, y],
                    wave_ss.at[d, 1, e, h], wave_rs.at[d, 1, e, h], (z * 8 + k, lev),
                )
        if h == 0:
            dst[e, 0, z] = by[e, :, z]
        else:
            dst[e, 1, :, y] = bz[e, :, y]

    def legendre(e, h):
        arrived(recv_f.at[e, pl.ds(2 * h, 2), pl.ds(0, 7)], lev_rs.at[0, e, h])
        parts = []
        for s in (2 * h, 2 * h + 1):
            out = dot(leg_t[s], recv_f[e, s].reshape(256, 128))
            parts.append(out.reshape(32, 8, 128))
        low, high = interleave(*parts)
        pairs = jnp.stack([low, high], axis=1).reshape(8, 8, 8, 128)
        a1[e, h] = pairs.astype(BF16)
        first_hop(0, e, h, a1, b1y, b1z)

    def gather_leg(h):
        arrived(leg.at[pl.ds(2 * h, 2), pl.ds(0, 7)], leg_rs.at[h])
        for s in (2 * h, 2 * h + 1):
            leg_t[s] = leg[s].reshape(256, 256).T

    gather_leg(0)
    legendre(0, 0)
    gather_leg(1)
    legendre(0, 1)
    second_hop(0, 0, 0, b1y, b1z, c1)
    legendre(1, 0)
    second_hop(0, 0, 1, b1y, b1z, c1)
    legendre(1, 1)
    second_hop(0, 1, 0, b1y, b1z, c1)
    second_hop(0, 1, 1, b1y, b1z, c1)

    ins[3].wait()
    ins[4].wait()
    diagonal = lax.broadcasted_iota(jnp.int32, (64, 64), 0) == lax.broadcasted_iota(
        jnp.int32, (64, 64), 1
    )
    bands = lax.broadcasted_iota(jnp.int32, (8, 64), 0)
    scales = []
    for t in range(4):
        line = jnp.sum(jnp.where(bands == band_s[t], scale[...], 0.0), axis=0, keepdims=True)
        square = jnp.where(diagonal, jnp.broadcast_to(line, (64, 64)), 0.0)
        scales.append(jnp.sum(square, axis=1, keepdims=True))
    first_half = lax.broadcasted_iota(jnp.int32, (256, 128), 1) < 64

    def grid_point(e):
        arrived(c1.at[e, 0, pl.ds(0, 7)], wave_rs.at[0, 1, e, 0])
        arrived(c1.at[e, 1, pl.ds(0, 7)], wave_rs.at[0, 1, e, 1])
        for h in range(2):
            xf[h] = c1[e, h].astype(F32).reshape(512, 128)
        backs = []
        for t in range(4):
            x = jnp.concatenate([xf[h, pl.ds(t, 128, stride=4), :] for h in range(2)], axis=0)
            xt = x.T.astype(BF16)
            got = dot(xt[0:64], table[t, 0]) + dot(xt[64:128], table[t, 1])
            made = (got * scales[t]).astype(BF16)
            inc[e, t] = made
            heavy = (made.astype(F32) * obs[t].astype(F32) * scales[t]).astype(BF16)
            twice = jnp.concatenate([heavy, heavy], axis=0)
            real = dot(table[t, 0], twice, ((1,), (1,)))
            imag = dot(table[t, 1], twice, ((1,), (1,)))
            backs.append(jnp.where(first_half, real, imag))
        for t in range(4):
            for h in range(2):
                xf[h, pl.ds(t, 128, stride=4), :] = backs[t][h * 128 : h * 128 + 128]
        for h in range(2):
            a2[e, h] = xf[h].reshape(8, 8, 8, 128).astype(BF16)
            first_hop(1, e, h, a2, b2y, b2z)
        pltpu.make_async_copy(inc.at[e], inc_h.at[e], out_sem.at[0, e]).start()

    grid_point(0)
    grid_point(1)
    for e in range(2):
        for h in range(2):
            second_hop(1, e, h, b2y, b2z, c2)

    def legendre_back(e, h):
        if h == 0:
            arrived(c2.at[e, 0, pl.ds(0, 7)], wave_rs.at[1, 1, e, h])
        else:
            arrived(c2.at[e, 1, pl.ds(0, 7)], wave_rs.at[1, 1, e, h])
        rows = c2[e, h].astype(F32).reshape(32, 2, 8, 128)
        for i, piece in enumerate(interleave(rows[:, 0], rows[:, 1])):
            s = 2 * h + i
            out = dot(leg[s].reshape(256, 256), piece.reshape(256, 128).astype(BF16))
            out = out.astype(BF16).reshape(8, 32, 128)
            for v in range(8):
                send_b[v, e, s] = out[v]
        for i in FAR_FIRST:
            v = lev_peer(i)
            remote(
                send_b.at[v, e, pl.ds(2 * h, 2)], recv_b.at[lev, e, pl.ds(2 * h, 2)],
                lev_ss.at[1, e, h], lev_rs.at[1, e, h], (wave, v),
            )
        for s in (2 * h, 2 * h + 1):
            recv_b[lev, e, s] = send_b[lev, e, s]

    def vertical_back(e):
        for h in range(2):
            arrived(recv_b.at[pl.ds(0, 7), e, pl.ds(2 * h, 2)], lev_rs.at[1, e, h])
        for a in range(VARIABLES):
            both = [recv_b[2 * a + half, e].reshape(128, 128) for half in range(2)]
            out = jnp.zeros((128, 256), F32)
            for b in range(COV_BANDS):
                x = jnp.concatenate([part * mask[b] for part in both], axis=1)
                out = out + dot(x, mix[b * VARIABLES + a])
            out = out.astype(BF16)
            grad[e, :, a * 128 : a * 128 + 128] = out[:, 0:128]
            grad[e, :, 512 + a * 128 : 640 + a * 128] = out[:, 128:256]
        pltpu.make_async_copy(grad.at[e], grad_h.at[e], out_sem.at[1, e]).start()

    for h in range(2):
        legendre_back(0, h)
    for h in range(2):
        legendre_back(1, h)
    vertical_back(0)
    vertical_back(1)

    for h in range(2):
        arrived(leg.at[pl.ds(2 * h, 2), pl.ds(0, 7)], leg_ss.at[h])
        for e in range(2):
            for d in range(2):
                arrived(recv_f.at[e, pl.ds(2 * h, 2), pl.ds(0, 7)], lev_ss.at[d, e, h])
                for hop in range(2):
                    arrived(b1y.at[e, pl.ds(0, 7)], wave_ss.at[d, hop, e, h])
    for e in range(2):
        pltpu.make_async_copy(inc.at[e], inc_h.at[e], out_sem.at[0, e]).wait()
        pltpu.make_async_copy(grad.at[e], grad_h.at[e], out_sem.at[1, e]).wait()


def shards(control, wave_of_slot, legendre, vertical, points, lat_band, grid_scale, obs_weight):
    members, slots, rows_dev = control.shape[0], control.shape[1], control.shape[2]
    flat = control.reshape(members * slots * rows_dev, 1024)
    smem = pl.BlockSpec(memory_space=pltpu.SMEM)
    vmem = pl.BlockSpec(memory_space=pltpu.VMEM)
    anywhere = pl.BlockSpec(memory_space=pl.ANY)
    wide = (2, 2, 8, 8, 8, 128)
    hop = (2, 8, 8, 8, 128)
    increment, gradient = pl.pallas_call(
        kernel,
        out_shape=(
            jax.ShapeDtypeStruct((2, 4, 64, 512), BF16),
            jax.ShapeDtypeStruct((2, 128, 1024), BF16),
        ),
        in_specs=[smem, smem, smem, vmem] + [anywhere] * 5,
        out_specs=(anywhere, anywhere),
        scratch_shapes=[
            pltpu.VMEM((256, 1024), BF16),
            pltpu.VMEM((16, 128, 128), BF16),
            pltpu.VMEM((4, 32, 256), BF16),
            pltpu.VMEM((8, 64), F32),
            pltpu.VMEM((4, 64, 512), BF16),
            pltpu.VMEM((2, 4, 64, 512), BF16),
            pltpu.VMEM((2, 128, 1024), BF16),
            pltpu.VMEM((4, 128, 128), BF16),
            pltpu.VMEM((16, 256, 256), BF16),
            pltpu.VMEM((8, 2, 4, 32, 128), BF16),
            pltpu.VMEM((2, 4, 8, 32, 128), BF16),
            pltpu.VMEM((4, 8, 32, 256), BF16),
            pltpu.VMEM((4, 256, 256), BF16),
            pltpu.VMEM((256, 128), F32),
            pltpu.VMEM((4, 2, 256, 512), BF16),
            pltpu.VMEM(wide, BF16),
            pltpu.VMEM(hop, BF16),
            pltpu.VMEM(hop, BF16),
            pltpu.VMEM(wide, BF16),
            pltpu.VMEM((2, 512, 128), F32),
            pltpu.VMEM(wide, BF16),
            pltpu.VMEM(hop, BF16),
            pltpu.VMEM(hop, BF16),
            pltpu.VMEM(wide, BF16),
            pltpu.VMEM((8, 2, 4, 32, 128), BF16),
            pltpu.VMEM((8, 2, 4, 32, 128), BF16),
            pltpu.SemaphoreType.DMA((5,)),
            pltpu.SemaphoreType.DMA((2, 2)),
            pltpu.SemaphoreType.DMA((2,)),
            pltpu.SemaphoreType.DMA((2,)),
            pltpu.SemaphoreType.DMA((2, 2, 2)),
            pltpu.SemaphoreType.DMA((2, 2, 2)),
            pltpu.SemaphoreType.DMA((2, 2, 2, 2)),
            pltpu.SemaphoreType.DMA((2, 2, 2, 2)),
        ],
        compiler_params=pltpu.CompilerParams(
            collective_id=0, has_side_effects=True, vmem_limit_bytes=60_000_000
        ),
    )(
        wave_of_slot, points, lat_band, wave_of_slot.reshape(2, 128),
        flat, legendre, vertical.reshape(16, 128, 128), grid_scale, obs_weight,
    )
    return increment, gradient.reshape(control.shape)


def solution(mesh):
    in_specs = (
        P(None, "wave", "lev", None, None),
        P(),
        P("wave", "lev", None),
        P(),
        P("wave"),
        P("wave"),
        P(None, "lev"),
        P("wave", "lev", None),
    )
    out_specs = (P(None, "wave", "lev", None), P(None, "wave", "lev", None, None))
    return jax.shard_map(shards, mesh=mesh, in_specs=in_specs, out_specs=out_specs, check_vma=False)
```

```python
import functools

import jax
import jax.numpy as jnp
from jax import lax
from jax.experimental import pallas as pl
from jax.experimental.pallas import tpu as pltpu
from jax.sharding import PartitionSpec as P

WAVES = 256
LONGITUDES = 512
COV_BANDS = 4
VARIABLES = 4
MESH = pl.DeviceIdType.MESH
F32 = jnp.float32
BF16 = jnp.bfloat16
FAR_FIRST = (4, 3, 5, 2, 6, 1, 7)
SIN = (6.283185302498671, -41.34170040100665, 81.6051311559332, -76.70301094142194,
       42.02588917305049, -14.899698808670236, 3.237922486217859)
COS = (0.9999999998851921, -19.739208743292323, 64.93938906426658, -85.45665800487392,
       60.24212744331612, -26.404643265364264, 7.800052913395129, -1.453015691570865)


def polynomial(terms, s):
    value = jnp.full(s.shape, terms[-1], F32)
    for term in terms[-2::-1]:
        value = value * s + term
    return value


def dot(a, b, dims=((1,), (0,))):
    return lax.dot_general(a, b, (dims, ((), ())), preferred_element_type=F32)


def kernel(
    waves_s, points_s, band_s, waves_v, ctl, own_leg, ver, scale, obs,
    inc, grad,
    mask, mix, send_f, recv_f, leg, leg_t, wcol, table,
    a1, c1, xf, a2, c2, send_b, recv_b,
    ready, leg_ss, leg_rs, lev_ss, lev_rs, wave_ss, wave_rs,
):
    wave = lax.axis_index("wave")
    lev = lax.axis_index("lev")
    z = wave // 8
    y = lax.rem(wave, 8)

    barrier = pltpu.get_barrier_semaphore()

    def along(i):
        return (
            (wave, lax.rem(lev + i, 8)),
            (z * 8 + lax.rem(y + i, 8), lev),
            (lax.rem(z + i, 8) * 8 + y, lev),
        )

    for i in FAR_FIRST:
        for who in along(i):
            pl.semaphore_signal(barrier, inc=1, device_id=who, device_id_type=MESH)

    row = lax.broadcasted_iota(jnp.int32, (128, 128), 0)
    slot = row // 32
    total = lev * 32 + lax.rem(row, 32)
    for s in range(4):
        total = total + jnp.where(slot == s, waves_s[wave * 4 + s], 0)
    band = jnp.minimum(total * COV_BANDS // WAVES, COV_BANDS - 1)
    for b in range(COV_BANDS):
        chosen = (total <= WAVES - 1) & (band == b)
        mask[b] = jnp.where(chosen, 1.0, 0.0).astype(BF16)

    def lay(i, carry):
        zero = jnp.zeros((64, 128), BF16)
        v = ver[i]
        for half in range(2):
            piece = v[half * 64 : half * 64 + 64]
            mix[i, half * 128 : half * 128 + 64, 0:128] = piece
            mix[i, half * 128 : half * 128 + 64, 128:256] = zero
            mix[i, half * 128 + 64 : half * 128 + 128, 0:128] = zero
            mix[i, half * 128 + 64 : half * 128 + 128, 128:256] = piece
        return carry

    lax.fori_loop(0, COV_BANDS * VARIABLES, lay, 0)

    for a in range(VARIABLES):
        both = [ctl[:, a * 128 : a * 128 + 128], ctl[:, 512 + a * 128 : 640 + a * 128]]
        out = jnp.zeros((256, 256), F32)
        for b in range(COV_BANDS):
            m = jnp.concatenate([mask[b], mask[b]], axis=0)
            x = jnp.concatenate([part * m for part in both], axis=1)
            out = out + dot(x, mix[b * VARIABLES + a], ((1,), (1,)))
        out = out.astype(BF16)
        for half in range(2):
            send_f[2 * a + half] = out[:, half * 128 : half * 128 + 128].reshape(2, 4, 32, 128)

    pl.semaphore_wait(barrier, 21)
    for i in FAR_FIRST:
        pl.semaphore_signal(
            ready, inc=1, device_id=(lax.rem(z + i, 8) * 8 + y, lev), device_id_type=MESH
        )

    def lev_peer(i):
        return lax.rem(lev + i, 8)

    def remote(src, dst, ss, rs, who):
        pltpu.make_async_remote_copy(
            src, dst, ss, rs, device_id=who, device_id_type=MESH
        ).start()

    def arrived(buffer, sem):
        pltpu.make_async_copy(buffer, buffer, sem).wait()

    def send_leg(h):
        for i in FAR_FIRST:
            remote(
                own_leg.at[pl.ds(2 * h, 2)], leg.at[pl.ds(2 * h, 2), lev],
                leg_ss.at[h], leg_rs.at[h], (wave, lev_peer(i)),
            )

    def send_spec(e, h):
        for i in FAR_FIRST:
            v = lev_peer(i)
            remote(
                send_f.at[v, e, pl.ds(2 * h, 2)], recv_f.at[e, pl.ds(2 * h, 2), lev],
                lev_ss.at[0, e, h], lev_rs.at[0, e, h], (wave, v),
            )

    send_leg(0)
    send_spec(0, 0)
    send_leg(1)
    send_spec(0, 1)
    send_spec(1, 0)
    send_spec(1, 1)
    for s in range(4):
        leg[s, lev] = own_leg[s]
        for e in range(2):
            recv_f[e, s, lev] = send_f[lev, e, s]

    place = lax.broadcasted_iota(jnp.int32, (256, 128), 0)
    wanted = lax.rem(place, 128) // 2 * 4 + place // 128 * 2 + lax.rem(place, 2)
    lane = lax.broadcasted_iota(jnp.int32, (256, 128), 1)
    found = jnp.zeros((256, 128), F32)
    for i in range(2):
        numbers = waves_v[i : i + 1, :].astype(F32)
        found = found + jnp.where(wanted == lane + i * 128, numbers, 0.0)
    wcol[...] = jnp.broadcast_to(jnp.sum(found, axis=1, keepdims=True), (256, 128))

    for t in range(4):
        count = jnp.full((16, LONGITUDES), points_s[t], jnp.int32).astype(F32)
        inverse = 1.0 / count

        def rows_of_table(i, carry, t=t, count=count, inverse=inverse):
            at = pl.multiple_of(i * 16, 16)
            w = wcol[pl.ds(at, 16), :]
            w = jnp.concatenate([w, w, w, w], axis=1)
            j = lax.broadcasted_iota(jnp.int32, (16, LONGITUDES), 1).astype(F32)
            product = w * j
            turns = jnp.floor(product * inverse + 0.5)
            x = (product - turns * count) * inverse
            s = x * x
            factor = jnp.where(w == 0.0, 1.0, 2.0) * (1.0 / 32.0)
            factor = jnp.where(j < count, factor, 0.0)
            table[t, 0, pl.ds(at, 16), :] = (factor * polynomial(COS, s)).astype(BF16)
            table[t, 1, pl.ds(at, 16), :] = (-factor * (x * polynomial(SIN, s))).astype(BF16)
            return carry

        lax.fori_loop(0, 16, rows_of_table, 0)

    sub = lax.broadcasted_iota(jnp.int32, (32, 8, 128), 1)

    def interleave(p, q):
        return (
            jnp.where(sub < 4, p, pltpu.roll(q, 4, 1)),
            jnp.where(sub < 4, pltpu.roll(p, 4, 1), q),
        )

    def exchange(d, e, h, src, dst):
        def one(i, carry):
            k = lax.rem(wave + i, 64)
            remote(
                src.at[e, h, k], dst.at[e, h, wave],
                wave_ss.at[d, e, h], wave_rs.at[d, e, h], (k, lev),
            )
            return carry

        lax.fori_loop(1, 64, one, 0, unroll=7)
        dst[e, h, wave] = src[e, h, wave]

    def exchanged(d, e, h, dst):
        arrived(dst.at[e, h, pl.ds(0, 63)], wave_rs.at[d, e, h])

    def legendre(e, h):
        arrived(recv_f.at[e, pl.ds(2 * h, 2), pl.ds(0, 7)], lev_rs.at[0, e, h])
        parts = []
        for s in (2 * h, 2 * h + 1):
            out = dot(leg_t[s], recv_f[e, s].reshape(256, 128))
            parts.append(out.reshape(32, 8, 128))
        low, high = interleave(*parts)
        pairs = jnp.stack([low, high], axis=1).reshape(64, 8, 128)
        a1[e, h] = pairs.astype(BF16)
        exchange(0, e, h, a1, c1)

    def gather_leg(h):
        arrived(leg.at[pl.ds(2 * h, 2), pl.ds(0, 7)], leg_rs.at[h])
        for s in (2 * h, 2 * h + 1):
            leg_t[s] = leg[s].reshape(256, 256).T

    gather_leg(0)
    pl.semaphore_wait(ready, 7)
    legendre(0, 0)
    gather_leg(1)
    legendre(0, 1)
    legendre(1, 0)
    legendre(1, 1)

    diagonal = lax.broadcasted_iota(jnp.int32, (64, 64), 0) == lax.broadcasted_iota(
        jnp.int32, (64, 64), 1
    )
    bands = lax.broadcasted_iota(jnp.int32, (8, 64), 0)
    scales = []
    for t in range(4):
        line = jnp.sum(jnp.where(bands == band_s[t], scale[...], 0.0), axis=0, keepdims=True)
        square = jnp.where(diagonal, jnp.broadcast_to(line, (64, 64)), 0.0)
        scales.append(jnp.sum(square, axis=1, keepdims=True))
    first_half = lax.broadcasted_iota(jnp.int32, (256, 128), 1) < 64

    def grid_point(e):
        for h in range(2):
            exchanged(0, e, h, c1)
            xf[h] = c1[e, h].astype(F32).reshape(512, 128)
        backs = []
        for t in range(4):
            x = jnp.concatenate([xf[h, pl.ds(t, 128, stride=4), :] for h in range(2)], axis=0)
            xt = x.T.astype(BF16)
            got = dot(xt[0:64], table[t, 0]) + dot(xt[64:128], table[t, 1])
            made = (got * scales[t]).astype(BF16)
            inc[e, t] = made
            heavy = (made.astype(F32) * obs[t].astype(F32) * scales[t]).astype(BF16)
            twice = jnp.concatenate([heavy, heavy], axis=0)
            real = dot(table[t, 0], twice, ((1,), (1,)))
            imag = dot(table[t, 1], twice, ((1,), (1,)))
            backs.append(jnp.where(first_half, real, imag))
        for t in range(4):
            for h in range(2):
                xf[h, pl.ds(t, 128, stride=4), :] = backs[t][h * 128 : h * 128 + 128]
        for h in range(2):
            a2[e, h] = xf[h].reshape(64, 8, 128).astype(BF16)
            exchange(1, e, h, a2, c2)

    grid_point(0)
    grid_point(1)
    def legendre_back(e, h):
        exchanged(1, e, h, c2)
        rows = c2[e, h].astype(F32).reshape(32, 2, 8, 128)
        for i, piece in enumerate(interleave(rows[:, 0], rows[:, 1])):
            s = 2 * h + i
            out = dot(leg[s].reshape(256, 256), piece.reshape(256, 128).astype(BF16))
            out = out.astype(BF16).reshape(8, 32, 128)
            for v in range(8):
                send_b[v, e, s] = out[v]
        for i in FAR_FIRST:
            v = lev_peer(i)
            remote(
                send_b.at[v, e, pl.ds(2 * h, 2)], recv_b.at[lev, e, pl.ds(2 * h, 2)],
                lev_ss.at[1, e, h], lev_rs.at[1, e, h], (wave, v),
            )
        for s in (2 * h, 2 * h + 1):
            recv_b[lev, e, s] = send_b[lev, e, s]

    def vertical_back(e):
        for h in range(2):
            arrived(recv_b.at[pl.ds(0, 7), e, pl.ds(2 * h, 2)], lev_rs.at[1, e, h])
        for a in range(VARIABLES):
            both = [recv_b[2 * a + half, e].reshape(128, 128) for half in range(2)]
            out = jnp.zeros((128, 256), F32)
            for b in range(COV_BANDS):
                x = jnp.concatenate([part * mask[b] for part in both], axis=1)
                out = out + dot(x, mix[b * VARIABLES + a])
            out = out.astype(BF16)
            grad[e, :, a * 128 : a * 128 + 128] = out[:, 0:128]
            grad[e, :, 512 + a * 128 : 640 + a * 128] = out[:, 128:256]

    for h in range(2):
        legendre_back(0, h)
    for h in range(2):
        legendre_back(1, h)
    vertical_back(0)
    vertical_back(1)

    for h in range(2):
        arrived(leg.at[pl.ds(2 * h, 2), pl.ds(0, 7)], leg_ss.at[h])
        for e in range(2):
            for d in range(2):
                arrived(recv_f.at[e, pl.ds(2 * h, 2), pl.ds(0, 7)], lev_ss.at[d, e, h])
                arrived(c1.at[e, h, pl.ds(0, 63)], wave_ss.at[d, e, h])


def shards(control, wave_of_slot, legendre, vertical, points, lat_band, grid_scale, obs_weight):
    members, slots, rows_dev = control.shape[0], control.shape[1], control.shape[2]
    flat = control.reshape(members * slots * rows_dev, 1024)
    smem = pl.BlockSpec(memory_space=pltpu.SMEM)
    vmem = pl.BlockSpec(memory_space=pltpu.VMEM)
    wide = (2, 2, 64, 8, 128)
    increment, gradient = pl.pallas_call(
        kernel,
        out_shape=(
            jax.ShapeDtypeStruct((2, 4, 64, 512), BF16),
            jax.ShapeDtypeStruct((2, 128, 1024), BF16),
        ),
        in_specs=[smem] * 3 + [vmem] * 6,
        out_specs=(vmem, vmem),
        scratch_shapes=[
            pltpu.VMEM((4, 128, 128), BF16),
            pltpu.VMEM((16, 256, 256), BF16),
            pltpu.VMEM((8, 2, 4, 32, 128), BF16),
            pltpu.VMEM((2, 4, 8, 32, 128), BF16),
            pltpu.VMEM((4, 8, 32, 256), BF16),
            pltpu.VMEM((4, 256, 256), BF16),
            pltpu.VMEM((256, 128), F32),
            pltpu.VMEM((4, 2, 256, 512), BF16),
            pltpu.VMEM(wide, BF16),
            pltpu.VMEM(wide, BF16),
            pltpu.VMEM((2, 512, 128), F32),
            pltpu.VMEM(wide, BF16),
            pltpu.VMEM(wide, BF16),
            pltpu.VMEM((8, 2, 4, 32, 128), BF16),
            pltpu.VMEM((8, 2, 4, 32, 128), BF16),
            pltpu.SemaphoreType.REGULAR,
            pltpu.SemaphoreType.DMA((2,)),
            pltpu.SemaphoreType.DMA((2,)),
            pltpu.SemaphoreType.DMA((2, 2, 2)),
            pltpu.SemaphoreType.DMA((2, 2, 2)),
            pltpu.SemaphoreType.DMA((2, 2, 2)),
            pltpu.SemaphoreType.DMA((2, 2, 2)),
        ],
        compiler_params=pltpu.CompilerParams(
            collective_id=0, has_side_effects=True, vmem_limit_bytes=24_000_000
        ),
    )(
        wave_of_slot, points, lat_band, wave_of_slot.reshape(2, 128),
        flat, legendre, vertical.reshape(16, 128, 128), grid_scale, obs_weight,
    )
    return increment, gradient.reshape(control.shape)


def solution(mesh):
    in_specs = (
        P(None, "wave", "lev", None, None),
        P(),
        P("wave", "lev", None),
        P(),
        P("wave"),
        P("wave"),
        P(None, "lev"),
        P("wave", "lev", None),
    )
    out_specs = (P(None, "wave", "lev", None), P(None, "wave", "lev", None, None))
    return jax.shard_map(shards, mesh=mesh, in_specs=in_specs, out_specs=out_specs, check_vma=False)
```

```python
import functools

import jax
import jax.numpy as jnp
from jax import lax
from jax.experimental import pallas as pl
from jax.experimental.pallas import tpu as pltpu
from jax.sharding import PartitionSpec as P

WAVES = 256
LONGITUDES = 512
COV_BANDS = 4
VARIABLES = 4
MESH = pl.DeviceIdType.MESH
F32 = jnp.float32
BF16 = jnp.bfloat16
FAR_FIRST = (4, 3, 5, 2, 6, 1, 7)
SIN = (6.283185302498671, -41.34170040100665, 81.6051311559332, -76.70301094142194,
       42.02588917305049, -14.899698808670236, 3.237922486217859)
COS = (0.9999999998851921, -19.739208743292323, 64.93938906426658, -85.45665800487392,
       60.24212744331612, -26.404643265364264, 7.800052913395129, -1.453015691570865)


def polynomial(terms, s):
    value = jnp.full(s.shape, terms[-1], F32)
    for term in terms[-2::-1]:
        value = value * s + term
    return value


def dot(a, b, dims=((1,), (0,))):
    return lax.dot_general(a, b, (dims, ((), ())), preferred_element_type=F32)


def kernel(
    waves_h, points_h, band_h, ctl, own_leg, ver, scale, obs,
    inc, grad,
    waves_v, points_v, band_v, mask, mix, send_f, recv_f, leg, leg_t, wcol, table,
    a1, c1, xf, a2, c2, send_b, recv_b,
    in_sem, near, row_col, plane, leg_ss, leg_rs, leg_ps, lev_ss, lev_rs, wave_ss, wave_rs,
):
    wave = lax.axis_index("wave")
    lev = lax.axis_index("lev")
    z = wave // 8
    y = lax.rem(wave, 8)

    small = [
        pltpu.make_async_copy(src, dst, in_sem.at[i])
        for i, (src, dst) in enumerate(
            ((waves_h, waves_v), (points_h, points_v), (band_h, band_v))
        )
    ]
    for copy in small:
        copy.start()
    barrier = pltpu.get_barrier_semaphore()

    def greet(sem, who):
        pl.semaphore_signal(sem, inc=1, device_id=who, device_id_type=MESH)

    def on_y(i):
        return (z * 8 + lax.rem(y + i, 8), lev)

    def on_z(i):
        return (lax.rem(z + i, 8) * 8 + y, lev)

    def lev_peer(i):
        return lax.rem(lev + i, 8)

    for i in FAR_FIRST:
        greet(barrier, (wave, lev_peer(i)))
    for i in (1, 7):
        greet(barrier, on_y(i))
        greet(barrier, on_z(i))

    def lay(i, carry):
        zero = jnp.zeros((64, 128), BF16)
        v = ver[i]
        for half in range(2):
            piece = v[half * 64 : half * 64 + 64]
            mix[i, half * 128 : half * 128 + 64, 0:128] = piece
            mix[i, half * 128 : half * 128 + 64, 128:256] = zero
            mix[i, half * 128 + 64 : half * 128 + 128, 0:128] = zero
            mix[i, half * 128 + 64 : half * 128 + 128, 128:256] = piece
        return carry

    lax.fori_loop(0, COV_BANDS * VARIABLES, lay, 0)

    for copy in small:
        copy.wait()

    row = lax.broadcasted_iota(jnp.int32, (128, 128), 0)
    slot = row // 32
    total = lev * 32 + lax.rem(row, 32)
    numbers = jnp.concatenate([waves_v[0:1, :], waves_v[1:2, :]], axis=1)
    at_slot = lax.broadcasted_iota(jnp.int32, (1, WAVES), 1) - wave * 4
    for s in range(4):
        own = jnp.sum(jnp.where(at_slot == s, numbers.astype(F32), 0.0), axis=1, keepdims=True)
        total = total + jnp.where(slot == s, own.astype(jnp.int32), 0)
    band = jnp.minimum(total * COV_BANDS // WAVES, COV_BANDS - 1)
    for b in range(COV_BANDS):
        chosen = (total <= WAVES - 1) & (band == b)
        mask[b] = jnp.where(chosen, 1.0, 0.0).astype(BF16)

    for a in range(VARIABLES):
        both = [ctl[:, a * 128 : a * 128 + 128], ctl[:, 512 + a * 128 : 640 + a * 128]]
        out = jnp.zeros((256, 256), F32)
        for b in range(COV_BANDS):
            m = jnp.concatenate([mask[b], mask[b]], axis=0)
            x = jnp.concatenate([part * m for part in both], axis=1)
            out = out + dot(x, mix[b * VARIABLES + a], ((1,), (1,)))
        out = out.astype(BF16)
        for half in range(2):
            send_f[2 * a + half] = out[:, half * 128 : half * 128 + 128].reshape(2, 4, 32, 128)

    pl.semaphore_wait(barrier, 11)
    for i in (1, 7):
        greet(near, on_y(i))
        greet(near, on_z(i))

    def remote(src, dst, ss, rs, who):
        pltpu.make_async_remote_copy(
            src, dst, ss, rs, device_id=who, device_id_type=MESH
        ).start()

    def arrived(buffer, sem):
        pltpu.make_async_copy(buffer, buffer, sem).wait()

    partner = lev + 1 - 2 * lax.rem(lev, 2)

    def send_leg(h):
        two = pl.ds(2 * h, 2)
        for i in (4, 2, 6):
            remote(
                own_leg.at[two], leg.at[two, lev],
                leg_ss.at[h], leg_rs.at[h], (wave, lev_peer(i)),
            )
        remote(
            own_leg.at[two], leg.at[two, lev],
            leg_ss.at[h], leg_ps.at[h], (wave, partner),
        )

    def relay_leg(h):
        two = pl.ds(2 * h, 2)
        arrived(leg.at[two, pl.ds(0, 3)], leg_rs.at[h])
        for i in (2, 6, 4):
            v = lev_peer(i)
            remote(
                leg.at[two, v], leg.at[two, v],
                leg_ss.at[h], leg_ps.at[h], (wave, partner),
            )

    def send_spec(e, h):
        for i in FAR_FIRST:
            v = lev_peer(i)
            remote(
                send_f.at[v, e, pl.ds(2 * h, 2)], recv_f.at[e, pl.ds(2 * h, 2), lev],
                lev_ss.at[0, e, h], lev_rs.at[0, e, h], (wave, v),
            )

    send_leg(0)
    send_spec(0, 0)
    send_leg(1)
    send_spec(0, 1)
    send_spec(1, 0)
    send_spec(1, 1)
    for s in range(4):
        leg[s, lev] = own_leg[s]
        for e in range(2):
            recv_f[e, s, lev] = send_f[lev, e, s]

    place = lax.broadcasted_iota(jnp.int32, (256, 128), 0)
    wanted = lax.rem(place, 128) // 2 * 4 + place // 128 * 2 + lax.rem(place, 2)
    lane = lax.broadcasted_iota(jnp.int32, (256, 128), 1)
    found = jnp.zeros((256, 128), F32)
    for i in range(2):
        numbers = waves_v[i : i + 1, :].astype(F32)
        found = found + jnp.where(wanted == lane + i * 128, numbers, 0.0)
    wcol[...] = jnp.broadcast_to(jnp.sum(found, axis=1, keepdims=True), (256, 128))

    def make_table(t):
        count = jnp.broadcast_to(points_v[:, t : t + 1].astype(F32), (16, LONGITUDES))
        inverse = 1.0 / count

        def rows_of_table(i, carry):
            at = pl.multiple_of(i * 16, 16)
            w = wcol[pl.ds(at, 16), :]
            w = jnp.concatenate([w, w, w, w], axis=1)
            j = lax.broadcasted_iota(jnp.int32, (16, LONGITUDES), 1).astype(F32)
            product = w * j
            turns = jnp.floor(product * inverse + 0.5)
            x = (product - turns * count) * inverse
            s = x * x
            factor = jnp.where(w == 0.0, 1.0, 2.0) * (1.0 / 32.0)
            factor = jnp.where(j < count, factor, 0.0)
            table[t, 0, pl.ds(at, 16), :] = (factor * polynomial(COS, s)).astype(BF16)
            table[t, 1, pl.ds(at, 16), :] = (-factor * (x * polynomial(SIN, s))).astype(BF16)
            return carry

        lax.fori_loop(0, 16, rows_of_table, 0)

    make_table(0)
    make_table(1)
    pl.semaphore_wait(near, 4)
    for i in (2, 6, 1, 7):
        greet(row_col, on_y(i))
        greet(row_col, on_z(i))
    make_table(2)
    pl.semaphore_wait(row_col, 8)
    for i in FAR_FIRST:
        greet(plane, on_z(i))

    sub = lax.broadcasted_iota(jnp.int32, (32, 8, 128), 1)

    def interleave(p, q):
        return (
            jnp.where(sub < 4, p, pltpu.roll(q, 4, 1)),
            jnp.where(sub < 4, pltpu.roll(p, 4, 1), q),
        )

    def exchange(d, e, h, src, dst):
        def to(k):
            remote(
                src.at[e, h, k], dst.at[e, h, wave],
                wave_ss.at[d, e, h], wave_rs.at[d, e, h], (k, lev),
            )

        def one(n, carry):
            k = lax.rem(z + 4 + lax.rem(n, 2) * (n + 1) // 2 * 7 + (1 - lax.rem(n, 2)) * n // 2, 8)
            for i in FAR_FIRST + (0,):
                to(k * 8 + lax.rem(y + i, 8))
            return carry

        lax.fori_loop(0, 7, one, 0)
        for i in FAR_FIRST:
            to(z * 8 + lax.rem(y + i, 8))
        dst[e, h, wave] = src[e, h, wave]

    def exchanged(d, e, h, dst):
        arrived(dst.at[e, h, pl.ds(0, 63)], wave_rs.at[d, e, h])

    def legendre(e, h):
        arrived(recv_f.at[e, pl.ds(2 * h, 2), pl.ds(0, 7)], lev_rs.at[0, e, h])
        parts = []
        for s in (2 * h, 2 * h + 1):
            out = dot(leg_t[s], recv_f[e, s].reshape(256, 128))
            parts.append(out.reshape(32, 8, 128))
        low, high = interleave(*parts)
        pairs = jnp.stack([low, high], axis=1).reshape(64, 8, 128)
        a1[e, h] = pairs.astype(BF16)
        exchange(0, e, h, a1, c1)

    def gather_leg(h):
        arrived(leg.at[pl.ds(2 * h, 2), pl.ds(0, 4)], leg_ps.at[h])
        for s in (2 * h, 2 * h + 1):
            leg_t[s] = leg[s].reshape(256, 256).T

    relay_leg(0)
    make_table(3)
    gather_leg(0)
    pl.semaphore_wait(plane, 7)
    legendre(0, 0)
    relay_leg(1)
    gather_leg(1)
    legendre(0, 1)
    legendre(1, 0)
    legendre(1, 1)

    diagonal = lax.broadcasted_iota(jnp.int32, (64, 64), 0) == lax.broadcasted_iota(
        jnp.int32, (64, 64), 1
    )
    bands = lax.broadcasted_iota(jnp.int32, (8, 64), 0)
    scales = []
    for t in range(4):
        line = jnp.sum(jnp.where(bands == band_v[:, t : t + 1], scale[...], 0.0), axis=0, keepdims=True)
        square = jnp.where(diagonal, jnp.broadcast_to(line, (64, 64)), 0.0)
        scales.append(jnp.sum(square, axis=1, keepdims=True))
    first_half = lax.broadcasted_iota(jnp.int32, (256, 128), 1) < 64

    def grid_point(e):
        for h in range(2):
            exchanged(0, e, h, c1)
            xf[h] = c1[e, h].astype(F32).reshape(512, 128)
        backs = []
        for t in range(4):
            x = jnp.concatenate([xf[h, pl.ds(t, 128, stride=4), :] for h in range(2)], axis=0)
            xt = x.T.astype(BF16)
            got = dot(xt[0:64], table[t, 0]) + dot(xt[64:128], table[t, 1])
            made = (got * scales[t]).astype(BF16)
            inc[e, t] = made
            heavy = (made.astype(F32) * obs[t].astype(F32) * scales[t]).astype(BF16)
            twice = jnp.concatenate([heavy, heavy], axis=0)
            real = dot(table[t, 0], twice, ((1,), (1,)))
            imag = dot(table[t, 1], twice, ((1,), (1,)))
            backs.append(jnp.where(first_half, real, imag))
        for t in range(4):
            for h in range(2):
                xf[h, pl.ds(t, 128, stride=4), :] = backs[t][h * 128 : h * 128 + 128]
        for h in range(2):
            a2[e, h] = xf[h].reshape(64, 8, 128).astype(BF16)
            exchange(1, e, h, a2, c2)

    grid_point(0)
    grid_point(1)
    def legendre_back(e, h):
        exchanged(1, e, h, c2)
        rows = c2[e, h].astype(F32).reshape(32, 2, 8, 128)
        for i, piece in enumerate(interleave(rows[:, 0], rows[:, 1])):
            s = 2 * h + i
            out = dot(leg[s].reshape(256, 256), piece.reshape(256, 128).astype(BF16))
            out = out.astype(BF16).reshape(8, 32, 128)
            for v in range(8):
                send_b[v, e, s] = out[v]
        for i in FAR_FIRST:
            v = lev_peer(i)
            remote(
                send_b.at[v, e, pl.ds(2 * h, 2)], recv_b.at[lev, e, pl.ds(2 * h, 2)],
                lev_ss.at[1, e, h], lev_rs.at[1, e, h], (wave, v),
            )
        for s in (2 * h, 2 * h + 1):
            recv_b[lev, e, s] = send_b[lev, e, s]

    def vertical_back(e):
        for h in range(2):
            arrived(recv_b.at[pl.ds(0, 7), e, pl.ds(2 * h, 2)], lev_rs.at[1, e, h])
        for a in range(VARIABLES):
            both = [recv_b[2 * a + half, e].reshape(128, 128) for half in range(2)]
            out = jnp.zeros((128, 256), F32)
            for b in range(COV_BANDS):
                x = jnp.concatenate([part * mask[b] for part in both], axis=1)
                out = out + dot(x, mix[b * VARIABLES + a])
            out = out.astype(BF16)
            grad[e, :, a * 128 : a * 128 + 128] = out[:, 0:128]
            grad[e, :, 512 + a * 128 : 640 + a * 128] = out[:, 128:256]

    for h in range(2):
        legendre_back(0, h)
    for h in range(2):
        legendre_back(1, h)
    vertical_back(0)
    vertical_back(1)

    for h in range(2):
        arrived(leg.at[pl.ds(2 * h, 2), pl.ds(0, 7)], leg_ss.at[h])
        for e in range(2):
            for d in range(2):
                arrived(recv_f.at[e, pl.ds(2 * h, 2), pl.ds(0, 7)], lev_ss.at[d, e, h])
                arrived(c1.at[e, h, pl.ds(0, 63)], wave_ss.at[d, e, h])


def shards(control, wave_of_slot, legendre, vertical, points, lat_band, grid_scale, obs_weight):
    members, slots, rows_dev = control.shape[0], control.shape[1], control.shape[2]
    flat = control.reshape(members * slots * rows_dev, 1024)
    vmem = pl.BlockSpec(memory_space=pltpu.VMEM)
    hbm = pl.BlockSpec(memory_space=pltpu.HBM)
    wide = (2, 2, 64, 8, 128)
    increment, gradient = pl.pallas_call(
        kernel,
        out_shape=(
            jax.ShapeDtypeStruct((2, 4, 64, 512), BF16),
            jax.ShapeDtypeStruct((2, 128, 1024), BF16),
        ),
        in_specs=[hbm] * 3 + [vmem] * 5,
        out_specs=(vmem, vmem),
        scratch_shapes=[
            pltpu.VMEM((2, 128), jnp.int32),
            pltpu.VMEM((1, 4), jnp.int32),
            pltpu.VMEM((1, 4), jnp.int32),
            pltpu.VMEM((4, 128, 128), BF16),
            pltpu.VMEM((16, 256, 256), BF16),
            pltpu.VMEM((8, 2, 4, 32, 128), BF16),
            pltpu.VMEM((2, 4, 8, 32, 128), BF16),
            pltpu.VMEM((4, 8, 32, 256), BF16),
            pltpu.VMEM((4, 256, 256), BF16),
            pltpu.VMEM((256, 128), F32),
            pltpu.VMEM((4, 2, 256, 512), BF16),
            pltpu.VMEM(wide, BF16),
            pltpu.VMEM(wide, BF16),
            pltpu.VMEM((2, 512, 128), F32),
            pltpu.VMEM(wide, BF16),
            pltpu.VMEM(wide, BF16),
            pltpu.VMEM((8, 2, 4, 32, 128), BF16),
            pltpu.VMEM((8, 2, 4, 32, 128), BF16),
            pltpu.SemaphoreType.DMA((3,)),
            pltpu.SemaphoreType.REGULAR,
            pltpu.SemaphoreType.REGULAR,
            pltpu.SemaphoreType.REGULAR,
            pltpu.SemaphoreType.DMA((2,)),
            pltpu.SemaphoreType.DMA((2,)),
            pltpu.SemaphoreType.DMA((2,)),
            pltpu.SemaphoreType.DMA((2, 2, 2)),
            pltpu.SemaphoreType.DMA((2, 2, 2)),
            pltpu.SemaphoreType.DMA((2, 2, 2)),
            pltpu.SemaphoreType.DMA((2, 2, 2)),
        ],
        compiler_params=pltpu.CompilerParams(
            collective_id=0, has_side_effects=True, vmem_limit_bytes=24_000_000
        ),
    )(
        wave_of_slot.reshape(2, 128), points.reshape(1, 4), lat_band.reshape(1, 4), flat, legendre, vertical.reshape(16, 128, 128), grid_scale, obs_weight,
    )
    return increment, gradient.reshape(control.shape)


def solution(mesh):
    in_specs = (
        P(None, "wave", "lev", None, None),
        P(),
        P("wave", "lev", None),
        P(),
        P("wave"),
        P("wave"),
        P(None, "lev"),
        P("wave", "lev", None),
    )
    out_specs = (P(None, "wave", "lev", None), P(None, "wave", "lev", None, None))
    return jax.shard_map(shards, mesh=mesh, in_specs=in_specs, out_specs=out_specs, check_vma=False)
```

```python
import functools

import jax
import jax.numpy as jnp
from jax import lax
from jax.experimental import pallas as pl
from jax.experimental.pallas import tpu as pltpu
from jax.sharding import PartitionSpec as P

WAVES = 256
LONGITUDES = 512
COV_BANDS = 4
VARIABLES = 4
MESH = pl.DeviceIdType.MESH
F32 = jnp.float32
BF16 = jnp.bfloat16
FAR_FIRST = (4, 3, 5, 2, 6, 1, 7)
SIN = (6.283185302498671, -41.34170040100665, 81.6051311559332, -76.70301094142194,
       42.02588917305049, -14.899698808670236, 3.237922486217859)
COS = (0.9999999998851921, -19.739208743292323, 64.93938906426658, -85.45665800487392,
       60.24212744331612, -26.404643265364264, 7.800052913395129, -1.453015691570865)


def polynomial(terms, s):
    value = jnp.full(s.shape, terms[-1], F32)
    for term in terms[-2::-1]:
        value = value * s + term
    return value


def dot(a, b, dims=((1,), (0,))):
    return lax.dot_general(a, b, (dims, ((), ())), preferred_element_type=F32)


def kernel(
    waves_h, points_h, band_h, ctl_h, leg_h, ver_h, scale_h, obs_h,
    inc, grad,
    waves_v, points_v, band_v, ctl, own_leg, ver, scale, obs, rows, mask, mix, send_f, recv_f, leg, leg_t, wcol, table,
    a1, c1, part_sum, heavy, xf, a2, c2, send_b, recv_b,
    in_sem, row_col, plane, leg_ss, leg_rs, leg_ps, lev_ss, lev_rs, wave_ss, wave_rs,
):
    wave = lax.axis_index("wave")
    lev = lax.axis_index("lev")
    z = wave // 8
    y = lax.rem(wave, 8)

    pairs = (
        (ver_h, ver), (waves_h, waves_v), (ctl_h, ctl), (leg_h, own_leg),
        (points_h, points_v), (band_h, band_v), (scale_h, scale), (obs_h, obs),
    )
    ins = [pltpu.make_async_copy(src, dst, in_sem.at[i]) for i, (src, dst) in enumerate(pairs)]
    for copy in ins:
        copy.start()
    barrier = pltpu.get_barrier_semaphore()

    def greet(sem, who):
        pl.semaphore_signal(sem, inc=1, device_id=who, device_id_type=MESH)

    def on_y(i):
        return (z * 8 + lax.rem(y + i, 8), lev)

    def on_z(i):
        return (lax.rem(z + i, 8) * 8 + y, lev)

    def lev_peer(i):
        return lax.rem(lev + i, 8)

    for i in FAR_FIRST:
        greet(barrier, (wave, lev_peer(i)))
    for i in (2, 6, 1, 7):
        greet(barrier, on_y(i))
        greet(barrier, on_z(i))

    ins[0].wait()

    def lay(i, carry):
        zero = jnp.zeros((64, 128), BF16)
        v = ver[i]
        for half in range(2):
            piece = v[half * 64 : half * 64 + 64]
            mix[i, half * 128 : half * 128 + 64, 0:128] = piece
            mix[i, half * 128 : half * 128 + 64, 128:256] = zero
            mix[i, half * 128 + 64 : half * 128 + 128, 0:128] = zero
            mix[i, half * 128 + 64 : half * 128 + 128, 128:256] = piece
        return carry

    lax.fori_loop(0, COV_BANDS * VARIABLES, lay, 0)

    ins[1].wait()

    row = lax.broadcasted_iota(jnp.int32, (128, 128), 0)
    slot = row // 32
    total = lev * 32 + lax.rem(row, 32)
    numbers = jnp.concatenate([waves_v[0:1, :], waves_v[1:2, :]], axis=1)
    at_slot = lax.broadcasted_iota(jnp.int32, (1, WAVES), 1) - wave * 4
    for s in range(4):
        own = jnp.sum(jnp.where(at_slot == s, numbers.astype(F32), 0.0), axis=1, keepdims=True)
        total = total + jnp.where(slot == s, own.astype(jnp.int32), 0)
    band = jnp.minimum(total * COV_BANDS // WAVES, COV_BANDS - 1)
    for b in range(COV_BANDS):
        chosen = (total <= WAVES - 1) & (band == b)
        mask[b] = jnp.where(chosen, 1.0, 0.0).astype(BF16)

    ins[2].wait()
    rows[...] = ctl[...].astype(F32)
    for a in range(VARIABLES):
        both = [rows[pl.ds(2 * a + p, 256, stride=8), :].astype(BF16) for p in range(2)]
        out = jnp.zeros((256, 256), F32)
        for b in range(COV_BANDS):
            m = jnp.concatenate([mask[b], mask[b]], axis=0)
            x = jnp.concatenate([part * m for part in both], axis=1)
            out = out + dot(x, mix[b * VARIABLES + a], ((1,), (1,)))
        out = out.astype(BF16)
        for half in range(2):
            send_f[2 * a + half] = out[:, half * 128 : half * 128 + 128].reshape(2, 4, 32, 128)

    ins[3].wait()
    pl.semaphore_wait(barrier, 15)
    for i in (2, 6, 1, 7):
        greet(row_col, on_y(i))
        greet(row_col, on_z(i))

    def remote(src, dst, ss, rs, who):
        pltpu.make_async_remote_copy(
            src, dst, ss, rs, device_id=who, device_id_type=MESH
        ).start()

    def arrived(buffer, sem):
        pltpu.make_async_copy(buffer, buffer, sem).wait()

    partner = lev + 1 - 2 * lax.rem(lev, 2)

    def send_leg(h):
        two = pl.ds(2 * h, 2)
        for i in (4, 2, 6):
            remote(
                own_leg.at[two], leg.at[two, lev],
                leg_ss.at[h], leg_rs.at[h], (wave, lev_peer(i)),
            )
        remote(
            own_leg.at[two], leg.at[two, lev],
            leg_ss.at[h], leg_ps.at[h], (wave, partner),
        )

    def relay_leg(h):
        two = pl.ds(2 * h, 2)
        arrived(leg.at[two, pl.ds(0, 3)], leg_rs.at[h])
        for i in (2, 6, 4):
            v = lev_peer(i)
            remote(
                leg.at[two, v], leg.at[two, v],
                leg_ss.at[h], leg_ps.at[h], (wave, partner),
            )

    def send_spec(e, h):
        for i in FAR_FIRST:
            v = lev_peer(i)
            remote(
                send_f.at[v, e, pl.ds(2 * h, 2)], recv_f.at[e, pl.ds(2 * h, 2), lev],
                lev_ss.at[0, e, h], lev_rs.at[0, e, h], (wave, v),
            )

    send_leg(0)
    send_spec(0, 0)
    send_leg(1)
    send_spec(0, 1)
    send_spec(1, 0)
    send_spec(1, 1)
    for s in range(4):
        leg[s, lev] = own_leg[s]
        for e in range(2):
            recv_f[e, s, lev] = send_f[lev, e, s]

    place = lax.broadcasted_iota(jnp.int32, (256, 128), 0)
    wanted = lax.rem(place, 128) // 2 * 4 + place // 128 * 2 + lax.rem(place, 2)
    lane = lax.broadcasted_iota(jnp.int32, (256, 128), 1)
    found = jnp.zeros((256, 128), F32)
    for i in range(2):
        numbers = waves_v[i : i + 1, :].astype(F32)
        found = found + jnp.where(wanted == lane + i * 128, numbers, 0.0)
    wcol[...] = jnp.broadcast_to(jnp.sum(found, axis=1, keepdims=True), (256, 128))

    def make_table(t):
        count = jnp.broadcast_to(points_v[:, t : t + 1].astype(F32), (16, LONGITUDES))
        inverse = 1.0 / count

        def rows_of_table(i, carry):
            at = pl.multiple_of(i * 16, 16)
            w = wcol[pl.ds(at, 16), :]
            w = jnp.concatenate([w, w, w, w], axis=1)
            j = lax.broadcasted_iota(jnp.int32, (16, LONGITUDES), 1).astype(F32)
            product = w * j
            turns = jnp.floor(product * inverse + 0.5)
            x = (product - turns * count) * inverse
            s = x * x
            factor = jnp.where(w == 0.0, 1.0, 2.0) * (1.0 / 32.0)
            factor = jnp.where(j < count, factor, 0.0)
            to = pl.multiple_of(lax.rem(i, 8) * 16, 16)
            table[t, i // 8, 0, pl.ds(to, 16), :] = (factor * polynomial(COS, s)).astype(BF16)
            table[t, i // 8, 1, pl.ds(to, 16), :] = (-factor * (x * polynomial(SIN, s))).astype(BF16)
            return carry

        lax.fori_loop(0, 16, rows_of_table, 0)

    for copy in ins[4:]:
        copy.wait()
    make_table(0)
    make_table(1)
    pl.semaphore_wait(row_col, 8)
    for i in FAR_FIRST:
        greet(plane, on_z(i))

    sub = lax.broadcasted_iota(jnp.int32, (32, 8, 128), 1)

    def interleave(p, q):
        return (
            jnp.where(sub < 4, p, pltpu.roll(q, 4, 1)),
            jnp.where(sub < 4, pltpu.roll(p, 4, 1), q),
        )

    def exchange(d, e, h, src, dst):
        def to(k):
            remote(
                src.at[e, h, k], dst.at[e, h, wave],
                wave_ss.at[d, e, h], wave_rs.at[d, e, h], (k, lev),
            )

        def one(n, carry):
            k = lax.rem(z + 4 + lax.rem(n, 2) * (n + 1) // 2 * 7 + (1 - lax.rem(n, 2)) * n // 2, 8)
            for i in FAR_FIRST + (0,):
                to(k * 8 + lax.rem(y + i, 8))
            return carry

        lax.fori_loop(0, 7, one, 0)
        for i in FAR_FIRST:
            to(z * 8 + lax.rem(y + i, 8))
        dst[e, h, wave] = src[e, h, wave]

    def exchanged(d, e, h, dst):
        arrived(dst.at[e, h, pl.ds(0, 63)], wave_rs.at[d, e, h])

    def legendre(e, h):
        arrived(recv_f.at[e, pl.ds(2 * h, 2), pl.ds(0, 7)], lev_rs.at[0, e, h])
        parts = []
        for s in (2 * h, 2 * h + 1):
            out = dot(leg_t[s], recv_f[e, s].reshape(256, 128))
            parts.append(out.reshape(32, 8, 128))
        low, high = interleave(*parts)
        pairs = jnp.stack([low, high], axis=1).reshape(64, 8, 128)
        a1[e, h] = pairs.astype(BF16)
        exchange(0, e, h, a1, c1)

    def gather_leg(h):
        arrived(leg.at[pl.ds(2 * h, 2), pl.ds(0, 4)], leg_ps.at[h])
        for s in (2 * h, 2 * h + 1):
            leg_t[s] = leg[s].reshape(256, 256).T

    make_table(2)
    relay_leg(0)
    make_table(3)
    gather_leg(0)
    pl.semaphore_wait(plane, 7)
    legendre(0, 0)
    relay_leg(1)
    gather_leg(1)
    legendre(0, 1)
    legendre(1, 0)
    legendre(1, 1)

    diagonal = lax.broadcasted_iota(jnp.int32, (64, 64), 0) == lax.broadcasted_iota(
        jnp.int32, (64, 64), 1
    )
    bands = lax.broadcasted_iota(jnp.int32, (8, 64), 0)
    scales = []
    for t in range(4):
        line = jnp.sum(jnp.where(bands == band_v[:, t : t + 1], scale[...], 0.0), axis=0, keepdims=True)
        square = jnp.where(diagonal, jnp.broadcast_to(line, (64, 64)), 0.0)
        scales.append(jnp.sum(square, axis=1, keepdims=True))
    first_half = lax.broadcasted_iota(jnp.int32, (128, 128), 1) < 64

    def synthesis(h, t):
        x = xf[h, pl.ds(t, 128, stride=4), :].T.astype(BF16)
        x = jnp.concatenate([x[0:64], x[64:128]], axis=1)
        return dot(x, table[t, h].reshape(256, LONGITUDES))

    def analysis(e, h):
        for t in range(4):
            out = dot(table[t, h].reshape(256, LONGITUDES), heavy[t], ((1,), (1,)))
            xf[h, pl.ds(t, 128, stride=4), :] = jnp.where(first_half, out[0:128], out[128:256])
        a2[e, h] = xf[h].reshape(64, 8, 128).astype(BF16)
        exchange(1, e, h, a2, c2)

    def grid_point(e):
        exchanged(0, e, 0, c1)
        xf[0] = c1[e, 0].astype(F32).reshape(512, 128)
        for t in range(4):
            part_sum[t] = synthesis(0, t)
        exchanged(0, e, 1, c1)
        xf[1] = c1[e, 1].astype(F32).reshape(512, 128)
        for t in range(4):
            got = part_sum[t] + synthesis(1, t)
            made = (got * scales[t]).astype(BF16)
            inc[e, t] = made
            weighted = (made.astype(F32) * obs[t].astype(F32) * scales[t]).astype(BF16)
            heavy[t, 0:64] = weighted
            heavy[t, 64:128] = weighted
        analysis(e, 0)
        analysis(e, 1)

    grid_point(0)
    grid_point(1)
    def legendre_back(e, h):
        exchanged(1, e, h, c2)
        got = c2[e, h].astype(F32).reshape(32, 2, 8, 128)
        for i, piece in enumerate(interleave(got[:, 0], got[:, 1])):
            s = 2 * h + i
            out = dot(leg[s].reshape(256, 256), piece.reshape(256, 128).astype(BF16))
            out = out.astype(BF16).reshape(8, 32, 128)
            for v in range(8):
                send_b[v, e, s] = out[v]
        for i in FAR_FIRST:
            v = lev_peer(i)
            remote(
                send_b.at[v, e, pl.ds(2 * h, 2)], recv_b.at[lev, e, pl.ds(2 * h, 2)],
                lev_ss.at[1, e, h], lev_rs.at[1, e, h], (wave, v),
            )
        for s in (2 * h, 2 * h + 1):
            recv_b[lev, e, s] = send_b[lev, e, s]

    def vertical_back(e):
        for h in range(2):
            arrived(recv_b.at[pl.ds(0, 7), e, pl.ds(2 * h, 2)], lev_rs.at[1, e, h])
        for a in range(VARIABLES):
            both = [recv_b[2 * a + half, e].reshape(128, 128) for half in range(2)]
            out = jnp.zeros((128, 256), F32)
            for b in range(COV_BANDS):
                x = jnp.concatenate([part * mask[b] for part in both], axis=1)
                out = out + dot(x, mix[b * VARIABLES + a])
            for p in range(2):
                rows[pl.ds(1024 * e + 2 * a + p, 128, stride=8), :] = out[:, p * 128 : p * 128 + 128]
        grad[pl.ds(1024 * e, 1024), :] = rows[pl.ds(1024 * e, 1024), :].astype(BF16)

    for h in range(2):
        legendre_back(0, h)
    for h in range(2):
        legendre_back(1, h)
    vertical_back(0)
    vertical_back(1)

    for h in range(2):
        arrived(leg.at[pl.ds(2 * h, 2), pl.ds(0, 7)], leg_ss.at[h])
        for e in range(2):
            for d in range(2):
                arrived(recv_f.at[e, pl.ds(2 * h, 2), pl.ds(0, 7)], lev_ss.at[d, e, h])
                arrived(c1.at[e, h, pl.ds(0, 63)], wave_ss.at[d, e, h])


def shards(control, wave_of_slot, legendre, vertical, points, lat_band, grid_scale, obs_weight):
    members, slots, rows_dev = control.shape[0], control.shape[1], control.shape[2]
    count = members * slots * rows_dev
    flat = control.reshape(count, 2, 4, 128).transpose(0, 2, 1, 3).reshape(count * 8, 128)
    vmem = pl.BlockSpec(memory_space=pltpu.VMEM)
    hbm = pl.BlockSpec(memory_space=pltpu.HBM)
    wide = (2, 2, 64, 8, 128)
    increment, gradient = pl.pallas_call(
        kernel,
        out_shape=(
            jax.ShapeDtypeStruct((2, 4, 64, 512), BF16),
            jax.ShapeDtypeStruct((2048, 128), BF16),
        ),
        in_specs=[hbm] * 8,
        out_specs=(vmem, vmem),
        scratch_shapes=[
            pltpu.VMEM((2, 128), jnp.int32),
            pltpu.VMEM((1, 4), jnp.int32),
            pltpu.VMEM((1, 4), jnp.int32),
            pltpu.VMEM((2048, 128), BF16),
            pltpu.VMEM((4, 32, 256), BF16),
            pltpu.VMEM((16, 128, 128), BF16),
            pltpu.VMEM((8, 64), F32),
            pltpu.VMEM((4, 64, 512), BF16),
            pltpu.VMEM((2048, 128), F32),
            pltpu.VMEM((4, 128, 128), BF16),
            pltpu.VMEM((16, 256, 256), BF16),
            pltpu.VMEM((8, 2, 4, 32, 128), BF16),
            pltpu.VMEM((2, 4, 8, 32, 128), BF16),
            pltpu.VMEM((4, 8, 32, 256), BF16),
            pltpu.VMEM((4, 256, 256), BF16),
            pltpu.VMEM((256, 128), F32),
            pltpu.VMEM((4, 2, 2, 128, 512), BF16),
            pltpu.VMEM(wide, BF16),
            pltpu.VMEM(wide, BF16),
            pltpu.VMEM((4, 64, 512), F32),
            pltpu.VMEM((4, 128, 512), BF16),
            pltpu.VMEM((2, 512, 128), F32),
            pltpu.VMEM(wide, BF16),
            pltpu.VMEM(wide, BF16),
            pltpu.VMEM((8, 2, 4, 32, 128), BF16),
            pltpu.VMEM((8, 2, 4, 32, 128), BF16),
            pltpu.SemaphoreType.DMA((8,)),
            pltpu.SemaphoreType.REGULAR,
            pltpu.SemaphoreType.REGULAR,
            pltpu.SemaphoreType.DMA((2,)),
            pltpu.SemaphoreType.DMA((2,)),
            pltpu.SemaphoreType.DMA((2,)),
            pltpu.SemaphoreType.DMA((2, 2, 2)),
            pltpu.SemaphoreType.DMA((2, 2, 2)),
            pltpu.SemaphoreType.DMA((2, 2, 2)),
            pltpu.SemaphoreType.DMA((2, 2, 2)),
        ],
        compiler_params=pltpu.CompilerParams(
            collective_id=0, has_side_effects=True, vmem_limit_bytes=24_000_000
        ),
    )(
        *(
            pltpu.with_memory_space_constraint(x, pltpu.HBM)
            for x in (
                wave_of_slot.reshape(2, 128), points.reshape(1, 4), lat_band.reshape(1, 4), flat,
                legendre, vertical.reshape(16, 128, 128), grid_scale, obs_weight,
            )
        )
    )
    gradient = gradient.reshape(count, 4, 2, 128).transpose(0, 2, 1, 3)
    return increment, gradient.reshape(control.shape)


def solution(mesh):
    in_specs = (
        P(None, "wave", "lev", None, None),
        P(),
        P("wave", "lev", None),
        P(),
        P("wave"),
        P("wave"),
        P(None, "lev"),
        P("wave", "lev", None),
    )
    out_specs = (P(None, "wave", "lev", None), P(None, "wave", "lev", None, None))
    return jax.shard_map(shards, mesh=mesh, in_specs=in_specs, out_specs=out_specs, check_vma=False)
```

```python
import functools

import jax
import jax.numpy as jnp
from jax import lax
from jax.experimental import pallas as pl
from jax.experimental.pallas import tpu as pltpu
from jax.sharding import PartitionSpec as P

WAVES = 256
LONGITUDES = 512
COV_BANDS = 4
VARIABLES = 4
MESH = pl.DeviceIdType.MESH
F32 = jnp.float32
BF16 = jnp.bfloat16
FAR_FIRST = (4, 3, 5, 2, 6, 1, 7)
SIN = (6.283185302498671, -41.34170040100665, 81.6051311559332, -76.70301094142194,
       42.02588917305049, -14.899698808670236, 3.237922486217859)
COS = (0.9999999998851921, -19.739208743292323, 64.93938906426658, -85.45665800487392,
       60.24212744331612, -26.404643265364264, 7.800052913395129, -1.453015691570865)


def polynomial(terms, s):
    value = jnp.full(s.shape, terms[-1], F32)
    for term in terms[-2::-1]:
        value = value * s + term
    return value


def dot(a, b, dims=((1,), (0,))):
    return lax.dot_general(a, b, (dims, ((), ())), preferred_element_type=F32)


def kernel(
    waves_h, points_h, band_h, ctl_h, leg_h, ver_h, scale_h, obs_h,
    inc, grad,
    waves_v, points_v, band_v, ctl, own_leg, ver, scale, obs, rows, mask, mix, send_f, recv_f, leg, leg_t, wcol, table,
    a1, c1, part_sum, heavy, xf, a2, c2, send_b, recv_b,
    in_sem, row_col, plane, leg_ss, leg_rs, leg_ps, lev_ss, lev_rs, wave_ss, wave_rs,
):
    wave = lax.axis_index("wave")
    lev = lax.axis_index("lev")
    z = wave // 8
    y = lax.rem(wave, 8)

    barrier = pltpu.get_barrier_semaphore()

    def greet(sem, who):
        pl.semaphore_signal(sem, inc=1, device_id=who, device_id_type=MESH)

    def on_y(i):
        return (z * 8 + lax.rem(y + i, 8), lev)

    def on_z(i):
        return (lax.rem(z + i, 8) * 8 + y, lev)

    def lev_peer(i):
        return lax.rem(lev + i, 8)

    for i in FAR_FIRST:
        greet(barrier, (wave, lev_peer(i)))
    pairs = (
        (ver_h, ver), (waves_h, waves_v), (ctl_h, ctl), (leg_h, own_leg),
        (points_h, points_v), (band_h, band_v), (scale_h, scale), (obs_h, obs),
    )
    ins = [pltpu.make_async_copy(src, dst, in_sem.at[i]) for i, (src, dst) in enumerate(pairs)]
    for copy in ins:
        copy.start()
    for i in (2, 6, 1, 7):
        greet(barrier, on_y(i))
        greet(barrier, on_z(i))

    ins[1].wait()

    row = lax.broadcasted_iota(jnp.int32, (128, 128), 0)
    slot = row // 32
    total = lev * 32 + lax.rem(row, 32)
    numbers = jnp.concatenate([waves_v[0:1, :], waves_v[1:2, :]], axis=1)
    at_slot = lax.broadcasted_iota(jnp.int32, (1, WAVES), 1) - wave * 4
    for s in range(4):
        own = jnp.sum(jnp.where(at_slot == s, numbers.astype(F32), 0.0), axis=1, keepdims=True)
        total = total + jnp.where(slot == s, own.astype(jnp.int32), 0)
    band = jnp.minimum(total * COV_BANDS // WAVES, COV_BANDS - 1)
    for b in range(COV_BANDS):
        chosen = (total <= WAVES - 1) & (band == b)
        mask[b] = jnp.where(chosen, 1.0, 0.0).astype(BF16)

    def remote(src, dst, ss, rs, who):
        pltpu.make_async_remote_copy(
            src, dst, ss, rs, device_id=who, device_id_type=MESH
        ).start()

    def arrived(buffer, sem):
        pltpu.make_async_copy(buffer, buffer, sem).wait()

    partner = lev + 1 - 2 * lax.rem(lev, 2)

    def send_leg(h):
        two = pl.ds(2 * h, 2)
        for i in (4, 2, 6):
            remote(
                own_leg.at[two], leg.at[two, lev],
                leg_ss.at[h], leg_rs.at[h], (wave, lev_peer(i)),
            )
        remote(
            own_leg.at[two], leg.at[two, lev],
            leg_ss.at[h], leg_ps.at[h], (wave, partner),
        )

    def relay_leg(h):
        two = pl.ds(2 * h, 2)
        arrived(leg.at[two, pl.ds(0, 3)], leg_rs.at[h])
        for i in (2, 6, 4):
            v = lev_peer(i)
            remote(
                leg.at[two, v], leg.at[two, v],
                leg_ss.at[h], leg_ps.at[h], (wave, partner),
            )

    def send_spec(e, h):
        for i in FAR_FIRST:
            v = lev_peer(i)
            remote(
                send_f.at[v, e, pl.ds(2 * h, 2)], recv_f.at[e, pl.ds(2 * h, 2), lev],
                lev_ss.at[0, e, h], lev_rs.at[0, e, h], (wave, v),
            )

    lane_low = lax.broadcasted_iota(jnp.int32, (128, 128), 1) < 64

    def vertical(e):
        for a in range(VARIABLES):
            x = [rows[pl.ds(1024 * e + 2 * a + p, 128, stride=8), :].astype(BF16) for p in range(2)]
            x = [jnp.concatenate([part * mask[b] for b in range(COV_BANDS)], axis=1) for part in x]
            matrices = [ver[b * VARIABLES + a] for b in range(COV_BANDS)]
            out = dot(
                jnp.concatenate(x, axis=0), jnp.concatenate(matrices, axis=1), ((1,), (1,))
            )
            real, imag = out[0:128], out[128:256]
            low = jnp.where(lane_low, real, pltpu.roll(imag, 64, 1))
            high = jnp.where(lane_low, pltpu.roll(real, 64, 1), imag)
            send_f[2 * a, e] = low.astype(BF16).reshape(4, 32, 128)
            send_f[2 * a + 1, e] = high.astype(BF16).reshape(4, 32, 128)

    ins[2].wait()
    rows[...] = ctl[...].astype(F32)
    ins[0].wait()
    vertical(0)
    ins[3].wait()
    pl.semaphore_wait(barrier, 15)
    for i in (2, 6, 1, 7):
        greet(row_col, on_y(i))
        greet(row_col, on_z(i))
    send_leg(0)
    send_spec(0, 0)
    send_leg(1)
    send_spec(0, 1)
    vertical(1)
    send_spec(1, 0)
    send_spec(1, 1)
    for s in range(4):
        leg[s, lev] = own_leg[s]
        for e in range(2):
            recv_f[e, s, lev] = send_f[lev, e, s]

    place = lax.broadcasted_iota(jnp.int32, (256, 128), 0)
    wanted = lax.rem(place, 128) // 2 * 4 + place // 128 * 2 + lax.rem(place, 2)
    lane = lax.broadcasted_iota(jnp.int32, (256, 128), 1)
    found = jnp.zeros((256, 128), F32)
    for i in range(2):
        numbers = waves_v[i : i + 1, :].astype(F32)
        found = found + jnp.where(wanted == lane + i * 128, numbers, 0.0)
    wcol[...] = jnp.broadcast_to(jnp.sum(found, axis=1, keepdims=True), (256, 128))

    def make_table(t):
        count = jnp.broadcast_to(points_v[:, t : t + 1].astype(F32), (16, LONGITUDES))
        inverse = 1.0 / count

        def rows_of_table(i, carry):
            at = pl.multiple_of(i * 16, 16)
            w = wcol[pl.ds(at, 16), :]
            w = jnp.concatenate([w, w, w, w], axis=1)
            j = lax.broadcasted_iota(jnp.int32, (16, LONGITUDES), 1).astype(F32)
            product = w * j
            turns = jnp.floor(product * inverse + 0.5)
            x = (product - turns * count) * inverse
            s = x * x
            factor = jnp.where(w == 0.0, 1.0, 2.0) * (1.0 / 32.0)
            factor = jnp.where(j < count, factor, 0.0)
            to = pl.multiple_of(lax.rem(i, 8) * 16, 16)
            table[t, i // 8, 0, pl.ds(to, 16), :] = (factor * polynomial(COS, s)).astype(BF16)
            table[t, i // 8, 1, pl.ds(to, 16), :] = (-factor * (x * polynomial(SIN, s))).astype(BF16)
            return carry

        lax.fori_loop(0, 16, rows_of_table, 0)

    def lay(i, carry):
        zero = jnp.zeros((64, 128), BF16)
        v = ver[i]
        for half in range(2):
            piece = v[half * 64 : half * 64 + 64]
            mix[i, half * 128 : half * 128 + 64, 0:128] = piece
            mix[i, half * 128 : half * 128 + 64, 128:256] = zero
            mix[i, half * 128 + 64 : half * 128 + 128, 0:128] = zero
            mix[i, half * 128 + 64 : half * 128 + 128, 128:256] = piece
        return carry

    lax.fori_loop(0, COV_BANDS * VARIABLES, lay, 0)

    for copy in ins[4:]:
        copy.wait()
    make_table(0)
    make_table(1)
    pl.semaphore_wait(row_col, 8)
    for i in FAR_FIRST:
        greet(plane, on_z(i))

    sub = lax.broadcasted_iota(jnp.int32, (32, 8, 128), 1)

    def interleave(p, q):
        return (
            jnp.where(sub < 4, p, pltpu.roll(q, 4, 1)),
            jnp.where(sub < 4, pltpu.roll(p, 4, 1), q),
        )

    def exchange(d, e, h, src, dst):
        def to(k):
            remote(
                src.at[e, h, k], dst.at[e, h, wave],
                wave_ss.at[d, e, h], wave_rs.at[d, e, h], (k, lev),
            )

        def one(n, carry):
            k = lax.rem(z + 4 + lax.rem(n, 2) * (n + 1) // 2 * 7 + (1 - lax.rem(n, 2)) * n // 2, 8)
            for i in FAR_FIRST + (0,):
                to(k * 8 + lax.rem(y + i, 8))
            return carry

        lax.fori_loop(0, 7, one, 0)
        for i in FAR_FIRST:
            to(z * 8 + lax.rem(y + i, 8))
        dst[e, h, wave] = src[e, h, wave]

    def exchanged(d, e, h, dst):
        arrived(dst.at[e, h, pl.ds(0, 63)], wave_rs.at[d, e, h])

    def legendre(e, h):
        arrived(recv_f.at[e, pl.ds(2 * h, 2), pl.ds(0, 7)], lev_rs.at[0, e, h])
        parts = []
        for s in (2 * h, 2 * h + 1):
            out = dot(leg_t[s], recv_f[e, s].reshape(256, 128))
            parts.append(out.reshape(32, 8, 128))
        low, high = interleave(*parts)
        pairs = jnp.stack([low, high], axis=1).reshape(64, 8, 128)
        a1[e, h] = pairs.astype(BF16)
        exchange(0, e, h, a1, c1)

    def gather_leg(h):
        arrived(leg.at[pl.ds(2 * h, 2), pl.ds(0, 4)], leg_ps.at[h])
        for s in (2 * h, 2 * h + 1):
            leg_t[s] = leg[s].reshape(256, 256).T

    make_table(2)
    relay_leg(0)
    make_table(3)
    gather_leg(0)
    pl.semaphore_wait(plane, 7)
    legendre(0, 0)
    relay_leg(1)
    gather_leg(1)
    legendre(0, 1)
    legendre(1, 0)
    legendre(1, 1)

    diagonal = lax.broadcasted_iota(jnp.int32, (64, 64), 0) == lax.broadcasted_iota(
        jnp.int32, (64, 64), 1
    )
    bands = lax.broadcasted_iota(jnp.int32, (8, 64), 0)
    scales = []
    for t in range(4):
        line = jnp.sum(jnp.where(bands == band_v[:, t : t + 1], scale[...], 0.0), axis=0, keepdims=True)
        square = jnp.where(diagonal, jnp.broadcast_to(line, (64, 64)), 0.0)
        scales.append(jnp.sum(square, axis=1, keepdims=True))
    first_half = lax.broadcasted_iota(jnp.int32, (128, 128), 1) < 64

    def synthesis(h, t):
        x = xf[h, pl.ds(t, 128, stride=4), :].T.astype(BF16)
        x = jnp.concatenate([x[0:64], x[64:128]], axis=1)
        return dot(x, table[t, h].reshape(256, LONGITUDES))

    def analysis(e, h):
        for t in range(4):
            out = dot(table[t, h].reshape(256, LONGITUDES), heavy[t], ((1,), (1,)))
            xf[h, pl.ds(t, 128, stride=4), :] = jnp.where(first_half, out[0:128], out[128:256])
        a2[e, h] = xf[h].reshape(64, 8, 128).astype(BF16)
        exchange(1, e, h, a2, c2)

    def grid_point(e):
        exchanged(0, e, 0, c1)
        xf[0] = c1[e, 0].astype(F32).reshape(512, 128)
        for t in range(4):
            part_sum[t] = synthesis(0, t)
        exchanged(0, e, 1, c1)
        xf[1] = c1[e, 1].astype(F32).reshape(512, 128)
        for t in range(4):
            got = part_sum[t] + synthesis(1, t)
            made = (got * scales[t]).astype(BF16)
            inc[e, t] = made
            weighted = (made.astype(F32) * obs[t].astype(F32) * scales[t]).astype(BF16)
            heavy[t, 0:64] = weighted
            heavy[t, 64:128] = weighted
        analysis(e, 0)
        analysis(e, 1)

    grid_point(0)
    grid_point(1)
    def legendre_back(e, h):
        exchanged(1, e, h, c2)
        got = c2[e, h].astype(F32).reshape(32, 2, 8, 128)
        for i, piece in enumerate(interleave(got[:, 0], got[:, 1])):
            s = 2 * h + i
            out = dot(leg[s].reshape(256, 256), piece.reshape(256, 128).astype(BF16))
            out = out.astype(BF16).reshape(8, 32, 128)
            for v in range(8):
                send_b[v, e, s] = out[v]
        for i in FAR_FIRST:
            v = lev_peer(i)
            remote(
                send_b.at[v, e, pl.ds(2 * h, 2)], recv_b.at[lev, e, pl.ds(2 * h, 2)],
                lev_ss.at[1, e, h], lev_rs.at[1, e, h], (wave, v),
            )
        for s in (2 * h, 2 * h + 1):
            recv_b[lev, e, s] = send_b[lev, e, s]

    def vertical_back(e):
        for h in range(2):
            arrived(recv_b.at[pl.ds(0, 7), e, pl.ds(2 * h, 2)], lev_rs.at[1, e, h])
        for a in range(VARIABLES):
            both = [recv_b[2 * a + half, e].reshape(128, 128) for half in range(2)]
            out = jnp.zeros((128, 256), F32)
            for b in range(COV_BANDS):
                x = jnp.concatenate([part * mask[b] for part in both], axis=1)
                out = out + dot(x, mix[b * VARIABLES + a])
            for p in range(2):
                rows[pl.ds(1024 * e + 2 * a + p, 128, stride=8), :] = out[:, p * 128 : p * 128 + 128]
        grad[pl.ds(1024 * e, 1024), :] = rows[pl.ds(1024 * e, 1024), :].astype(BF16)

    for h in range(2):
        legendre_back(0, h)
    for h in range(2):
        legendre_back(1, h)
    vertical_back(0)
    vertical_back(1)

    for h in range(2):
        arrived(leg.at[pl.ds(2 * h, 2), pl.ds(0, 7)], leg_ss.at[h])
        for e in range(2):
            for d in range(2):
                arrived(recv_f.at[e, pl.ds(2 * h, 2), pl.ds(0, 7)], lev_ss.at[d, e, h])
                arrived(c1.at[e, h, pl.ds(0, 63)], wave_ss.at[d, e, h])


def deliver(inc, grad, inc_h, grad_h, sem):
    copies = (
        pltpu.make_async_copy(inc, inc_h, sem.at[0]),
        pltpu.make_async_copy(grad, grad_h, sem.at[1]),
    )
    for copy in copies:
        copy.start()
    for copy in copies:
        copy.wait()


def shards(control, wave_of_slot, legendre, vertical, points, lat_band, grid_scale, obs_weight):
    members, slots, rows_dev = control.shape[0], control.shape[1], control.shape[2]
    count = members * slots * rows_dev
    flat = control.reshape(count, 2, 4, 128).transpose(0, 2, 1, 3).reshape(count * 8, 128)
    vmem = pl.BlockSpec(memory_space=pltpu.VMEM)
    hbm = pl.BlockSpec(memory_space=pltpu.HBM)
    wide = (2, 2, 64, 8, 128)
    increment, gradient = pl.pallas_call(
        kernel,
        out_shape=(
            jax.ShapeDtypeStruct((2, 4, 64, 512), BF16),
            jax.ShapeDtypeStruct((2048, 128), BF16),
        ),
        in_specs=[hbm] * 8,
        out_specs=(vmem, vmem),
        scratch_shapes=[
            pltpu.VMEM((2, 128), jnp.int32),
            pltpu.VMEM((1, 4), jnp.int32),
            pltpu.VMEM((1, 4), jnp.int32),
            pltpu.VMEM((2048, 128), BF16),
            pltpu.VMEM((4, 32, 256), BF16),
            pltpu.VMEM((16, 128, 128), BF16),
            pltpu.VMEM((8, 64), F32),
            pltpu.VMEM((4, 64, 512), BF16),
            pltpu.VMEM((2048, 128), F32),
            pltpu.VMEM((4, 128, 128), BF16),
            pltpu.VMEM((16, 256, 256), BF16),
            pltpu.VMEM((8, 2, 4, 32, 128), BF16),
            pltpu.VMEM((2, 4, 8, 32, 128), BF16),
            pltpu.VMEM((4, 8, 32, 256), BF16),
            pltpu.VMEM((4, 256, 256), BF16),
            pltpu.VMEM((256, 128), F32),
            pltpu.VMEM((4, 2, 2, 128, 512), BF16),
            pltpu.VMEM(wide, BF16),
            pltpu.VMEM(wide, BF16),
            pltpu.VMEM((4, 64, 512), F32),
            pltpu.VMEM((4, 128, 512), BF16),
            pltpu.VMEM((2, 512, 128), F32),
            pltpu.VMEM(wide, BF16),
            pltpu.VMEM(wide, BF16),
            pltpu.VMEM((8, 2, 4, 32, 128), BF16),
            pltpu.VMEM((8, 2, 4, 32, 128), BF16),
            pltpu.SemaphoreType.DMA((8,)),
            pltpu.SemaphoreType.REGULAR,
            pltpu.SemaphoreType.REGULAR,
            pltpu.SemaphoreType.DMA((2,)),
            pltpu.SemaphoreType.DMA((2,)),
            pltpu.SemaphoreType.DMA((2,)),
            pltpu.SemaphoreType.DMA((2, 2, 2)),
            pltpu.SemaphoreType.DMA((2, 2, 2)),
            pltpu.SemaphoreType.DMA((2, 2, 2)),
            pltpu.SemaphoreType.DMA((2, 2, 2)),
        ],
        compiler_params=pltpu.CompilerParams(
            collective_id=0, has_side_effects=True, vmem_limit_bytes=24_000_000
        ),
    )(
        *(
            pltpu.with_memory_space_constraint(x, pltpu.HBM)
            for x in (
                wave_of_slot.reshape(2, 128), points.reshape(1, 4), lat_band.reshape(1, 4), flat,
                legendre, vertical.reshape(16, 128, 128), grid_scale, obs_weight,
            )
        )
    )
    increment, gradient = pl.pallas_call(
        deliver,
        out_shape=(
            jax.ShapeDtypeStruct((2, 4, 64, 512), BF16),
            jax.ShapeDtypeStruct((2048, 128), BF16),
        ),
        in_specs=[vmem, vmem],
        out_specs=(hbm, hbm),
        scratch_shapes=[pltpu.SemaphoreType.DMA((2,))],
        compiler_params=pltpu.CompilerParams(vmem_limit_bytes=24_000_000),
    )(increment, gradient)
    gradient = gradient.reshape(count, 4, 2, 128).transpose(0, 2, 1, 3)
    return increment, gradient.reshape(control.shape)


def solution(mesh):
    in_specs = (
        P(None, "wave", "lev", None, None),
        P(),
        P("wave", "lev", None),
        P(),
        P("wave"),
        P("wave"),
        P(None, "lev"),
        P("wave", "lev", None),
    )
    out_specs = (P(None, "wave", "lev", None), P(None, "wave", "lev", None, None))
    return jax.shard_map(shards, mesh=mesh, in_specs=in_specs, out_specs=out_specs, check_vma=False)
```

```python
import functools

import jax
import jax.numpy as jnp
from jax import lax
from jax.experimental import pallas as pl
from jax.experimental.pallas import tpu as pltpu
from jax.sharding import PartitionSpec as P

WAVES = 256
LONGITUDES = 512
COV_BANDS = 4
VARIABLES = 4
MESH = pl.DeviceIdType.MESH
F32 = jnp.float32
BF16 = jnp.bfloat16
FAR_FIRST = (4, 3, 5, 2, 6, 1, 7)
BY_DISTANCE = sorted(
    ((i, j) for i in range(8) for j in range(8) if i + j > 0),
    key=lambda at: -min(at[0], 8 - at[0]) - min(at[1], 8 - at[1]),
)
SIN = (6.283185302498671, -41.34170040100665, 81.6051311559332, -76.70301094142194,
       42.02588917305049, -14.899698808670236, 3.237922486217859)
COS = (0.9999999998851921, -19.739208743292323, 64.93938906426658, -85.45665800487392,
       60.24212744331612, -26.404643265364264, 7.800052913395129, -1.453015691570865)


def polynomial(terms, s):
    value = jnp.full(s.shape, terms[-1], F32)
    for term in terms[-2::-1]:
        value = value * s + term
    return value


def dot(a, b, dims=((1,), (0,))):
    return lax.dot_general(a, b, (dims, ((), ())), preferred_element_type=F32)


def kernel(
    waves_h, points_h, band_h, ctl_h, leg_h, ver_h, scale_h, obs_h,
    inc, grad,
    waves_v, points_v, band_v, ctl, own_leg, ver, scale, obs, rows, mask, mix, send_f, recv_f, leg, leg_t, wcol, table,
    a1, c1, part_sum, heavy, xf, a2, c2, send_b, recv_b,
    in_sem, row_col, plane, leg_ss, leg_rs, leg_ps, lev_ss, lev_rs, wave_ss, wave_rs,
):
    wave = lax.axis_index("wave")
    lev = lax.axis_index("lev")
    z = wave // 8
    y = lax.rem(wave, 8)

    barrier = pltpu.get_barrier_semaphore()

    def greet(sem, who):
        pl.semaphore_signal(sem, inc=1, device_id=who, device_id_type=MESH)

    def on_y(i):
        return (z * 8 + lax.rem(y + i, 8), lev)

    def on_z(i):
        return (lax.rem(z + i, 8) * 8 + y, lev)

    def lev_peer(i):
        return lax.rem(lev + i, 8)

    for i in FAR_FIRST:
        greet(barrier, (wave, lev_peer(i)))
    pairs = (
        (ver_h, ver), (waves_h, waves_v), (ctl_h, ctl), (leg_h, own_leg),
        (points_h, points_v), (band_h, band_v), (scale_h, scale), (obs_h, obs),
    )
    ins = [pltpu.make_async_copy(src, dst, in_sem.at[i]) for i, (src, dst) in enumerate(pairs)]
    for copy in ins:
        copy.start()
    for i in (2, 6, 1, 7):
        greet(barrier, on_y(i))
        greet(barrier, on_z(i))

    ins[1].wait()

    row = lax.broadcasted_iota(jnp.int32, (128, 128), 0)
    slot = row // 32
    total = lev * 32 + lax.rem(row, 32)
    numbers = jnp.concatenate([waves_v[0:1, :], waves_v[1:2, :]], axis=1)
    at_slot = lax.broadcasted_iota(jnp.int32, (1, WAVES), 1) - wave * 4
    for s in range(4):
        own = jnp.sum(jnp.where(at_slot == s, numbers.astype(F32), 0.0), axis=1, keepdims=True)
        total = total + jnp.where(slot == s, own.astype(jnp.int32), 0)
    band = jnp.minimum(total * COV_BANDS // WAVES, COV_BANDS - 1)
    for b in range(COV_BANDS):
        chosen = (total <= WAVES - 1) & (band == b)
        mask[b] = jnp.where(chosen, 1.0, 0.0).astype(BF16)

    def remote(src, dst, ss, rs, who):
        pltpu.make_async_remote_copy(
            src, dst, ss, rs, device_id=who, device_id_type=MESH
        ).start()

    def arrived(buffer, sem):
        pltpu.make_async_copy(buffer, buffer, sem).wait()

    partner = lev + 1 - 2 * lax.rem(lev, 2)

    def send_leg(h):
        two = pl.ds(2 * h, 2)
        for i in (4, 2, 6):
            remote(
                own_leg.at[two], leg.at[two, lev],
                leg_ss.at[h], leg_rs.at[h], (wave, lev_peer(i)),
            )
        remote(
            own_leg.at[two], leg.at[two, lev],
            leg_ss.at[h], leg_ps.at[h], (wave, partner),
        )

    def relay_leg(h):
        two = pl.ds(2 * h, 2)
        arrived(leg.at[two, pl.ds(0, 3)], leg_rs.at[h])
        for i in (2, 6, 4):
            v = lev_peer(i)
            remote(
                leg.at[two, v], leg.at[two, v],
                leg_ss.at[h], leg_ps.at[h], (wave, partner),
            )

    def send_spec(e, h):
        for i in FAR_FIRST:
            v = lev_peer(i)
            remote(
                send_f.at[v, e, pl.ds(2 * h, 2)], recv_f.at[e, pl.ds(2 * h, 2), lev],
                lev_ss.at[0, e, h], lev_rs.at[0, e, h], (wave, v),
            )

    lane_low = lax.broadcasted_iota(jnp.int32, (128, 128), 1) < 64

    def vertical(e):
        for a in range(VARIABLES):
            x = [rows[pl.ds(1024 * e + 2 * a + p, 128, stride=8), :].astype(BF16) for p in range(2)]
            x = [jnp.concatenate([part * mask[b] for b in range(COV_BANDS)], axis=1) for part in x]
            matrices = [ver[b * VARIABLES + a] for b in range(COV_BANDS)]
            out = dot(
                jnp.concatenate(x, axis=0), jnp.concatenate(matrices, axis=1), ((1,), (1,))
            )
            real, imag = out[0:128], out[128:256]
            low = jnp.where(lane_low, real, pltpu.roll(imag, 64, 1))
            high = jnp.where(lane_low, pltpu.roll(real, 64, 1), imag)
            send_f[2 * a, e] = low.astype(BF16).reshape(4, 32, 128)
            send_f[2 * a + 1, e] = high.astype(BF16).reshape(4, 32, 128)

    ins[2].wait()
    rows[...] = ctl[...].astype(F32)
    ins[0].wait()
    vertical(0)
    ins[3].wait()
    pl.semaphore_wait(barrier, 15)
    for i in (2, 6, 1, 7):
        greet(row_col, on_y(i))
        greet(row_col, on_z(i))
    send_leg(0)
    send_spec(0, 0)
    send_leg(1)
    send_spec(0, 1)
    vertical(1)
    send_spec(1, 0)
    send_spec(1, 1)
    for s in range(4):
        leg[s, lev] = own_leg[s]
        for e in range(2):
            recv_f[e, s, lev] = send_f[lev, e, s]

    place = lax.broadcasted_iota(jnp.int32, (256, 128), 0)
    wanted = lax.rem(place, 128) // 2 * 4 + place // 128 * 2 + lax.rem(place, 2)
    lane = lax.broadcasted_iota(jnp.int32, (256, 128), 1)
    found = jnp.zeros((256, 128), F32)
    for i in range(2):
        numbers = waves_v[i : i + 1, :].astype(F32)
        found = found + jnp.where(wanted == lane + i * 128, numbers, 0.0)
    wcol[...] = jnp.broadcast_to(jnp.sum(found, axis=1, keepdims=True), (256, 128))

    def make_table(t):
        count = jnp.broadcast_to(points_v[:, t : t + 1].astype(F32), (16, LONGITUDES))
        inverse = 1.0 / count

        def rows_of_table(i, carry):
            at = pl.multiple_of(i * 16, 16)
            w = wcol[pl.ds(at, 16), :]
            w = jnp.concatenate([w, w, w, w], axis=1)
            j = lax.broadcasted_iota(jnp.int32, (16, LONGITUDES), 1).astype(F32)
            product = w * j
            turns = jnp.floor(product * inverse + 0.5)
            x = (product - turns * count) * inverse
            s = x * x
            factor = jnp.where(w == 0.0, 1.0, 2.0) * (1.0 / 32.0)
            factor = jnp.where(j < count, factor, 0.0)
            to = pl.multiple_of(lax.rem(i, 8) * 16, 16)
            table[t, i // 8, 0, pl.ds(to, 16), :] = (factor * polynomial(COS, s)).astype(BF16)
            table[t, i // 8, 1, pl.ds(to, 16), :] = (-factor * (x * polynomial(SIN, s))).astype(BF16)
            return carry

        lax.fori_loop(0, 16, rows_of_table, 0)

    def lay(i, carry):
        zero = jnp.zeros((64, 128), BF16)
        v = ver[i]
        for half in range(2):
            piece = v[half * 64 : half * 64 + 64]
            mix[i, half * 128 : half * 128 + 64, 0:128] = piece
            mix[i, half * 128 : half * 128 + 64, 128:256] = zero
            mix[i, half * 128 + 64 : half * 128 + 128, 0:128] = zero
            mix[i, half * 128 + 64 : half * 128 + 128, 128:256] = piece
        return carry

    lax.fori_loop(0, COV_BANDS * VARIABLES, lay, 0)

    for copy in ins[4:]:
        copy.wait()
    make_table(0)
    make_table(1)
    pl.semaphore_wait(row_col, 8)
    for i in FAR_FIRST:
        greet(plane, on_z(i))

    sub = lax.broadcasted_iota(jnp.int32, (32, 8, 128), 1)

    def interleave(p, q):
        return (
            jnp.where(sub < 4, p, pltpu.roll(q, 4, 1)),
            jnp.where(sub < 4, pltpu.roll(p, 4, 1), q),
        )

    def exchange(d, e, h, src, dst):
        def to(k):
            remote(
                src.at[e, h, k], dst.at[e, h, wave],
                wave_ss.at[d, e, h], wave_rs.at[d, e, h], (k, lev),
            )

        for i, j in BY_DISTANCE:
            to(lax.rem(z + i, 8) * 8 + lax.rem(y + j, 8))
        dst[e, h, wave] = src[e, h, wave]

    def exchanged(d, e, h, dst):
        arrived(dst.at[e, h, pl.ds(0, 63)], wave_rs.at[d, e, h])

    def legendre(e, h):
        arrived(recv_f.at[e, pl.ds(2 * h, 2), pl.ds(0, 7)], lev_rs.at[0, e, h])
        parts = []
        for s in (2 * h, 2 * h + 1):
            out = dot(leg_t[s], recv_f[e, s].reshape(256, 128))
            parts.append(out.reshape(32, 8, 128))
        low, high = interleave(*parts)
        pairs = jnp.stack([low, high], axis=1).reshape(64, 8, 128)
        a1[e, h] = pairs.astype(BF16)
        exchange(0, e, h, a1, c1)

    def gather_leg(h):
        arrived(leg.at[pl.ds(2 * h, 2), pl.ds(0, 4)], leg_ps.at[h])
        for s in (2 * h, 2 * h + 1):
            leg_t[s] = leg[s].reshape(256, 256).T

    make_table(2)
    relay_leg(0)
    make_table(3)
    gather_leg(0)
    pl.semaphore_wait(plane, 7)
    legendre(0, 0)
    relay_leg(1)
    gather_leg(1)
    legendre(0, 1)
    legendre(1, 0)
    legendre(1, 1)

    diagonal = lax.broadcasted_iota(jnp.int32, (64, 64), 0) == lax.broadcasted_iota(
        jnp.int32, (64, 64), 1
    )
    bands = lax.broadcasted_iota(jnp.int32, (8, 64), 0)
    scales = []
    for t in range(4):
        line = jnp.sum(jnp.where(bands == band_v[:, t : t + 1], scale[...], 0.0), axis=0, keepdims=True)
        square = jnp.where(diagonal, jnp.broadcast_to(line, (64, 64)), 0.0)
        scales.append(jnp.sum(square, axis=1, keepdims=True))
    first_half = lax.broadcasted_iota(jnp.int32, (128, 128), 1) < 64

    def synthesis(h, t):
        x = xf[h, pl.ds(t, 128, stride=4), :].T.astype(BF16)
        x = jnp.concatenate([x[0:64], x[64:128]], axis=1)
        return dot(x, table[t, h].reshape(256, LONGITUDES))

    def analysis(e, h):
        for t in range(4):
            out = dot(table[t, h].reshape(256, LONGITUDES), heavy[t], ((1,), (1,)))
            xf[h, pl.ds(t, 128, stride=4), :] = jnp.where(first_half, out[0:128], out[128:256])
        a2[e, h] = xf[h].reshape(64, 8, 128).astype(BF16)
        exchange(1, e, h, a2, c2)

    def grid_point(e):
        exchanged(0, e, 0, c1)
        xf[0] = c1[e, 0].astype(F32).reshape(512, 128)
        for t in range(4):
            part_sum[t] = synthesis(0, t)
        exchanged(0, e, 1, c1)
        xf[1] = c1[e, 1].astype(F32).reshape(512, 128)
        for t in range(4):
            got = part_sum[t] + synthesis(1, t)
            made = (got * scales[t]).astype(BF16)
            inc[e, t] = made
            weighted = (made.astype(F32) * obs[t].astype(F32) * scales[t]).astype(BF16)
            heavy[t, 0:64] = weighted
            heavy[t, 64:128] = weighted
        analysis(e, 0)
        analysis(e, 1)

    grid_point(0)
    grid_point(1)
    def legendre_back(e, h):
        exchanged(1, e, h, c2)
        got = c2[e, h].astype(F32).reshape(32, 2, 8, 128)
        for i, piece in enumerate(interleave(got[:, 0], got[:, 1])):
            s = 2 * h + i
            out = dot(leg[s].reshape(256, 256), piece.reshape(256, 128).astype(BF16))
            out = out.astype(BF16).reshape(8, 32, 128)
            for v in range(8):
                send_b[v, e, s] = out[v]
        for i in FAR_FIRST:
            v = lev_peer(i)
            remote(
                send_b.at[v, e, pl.ds(2 * h, 2)], recv_b.at[lev, e, pl.ds(2 * h, 2)],
                lev_ss.at[1, e, h], lev_rs.at[1, e, h], (wave, v),
            )
        for s in (2 * h, 2 * h + 1):
            recv_b[lev, e, s] = send_b[lev, e, s]

    def vertical_back(e):
        for h in range(2):
            arrived(recv_b.at[pl.ds(0, 7), e, pl.ds(2 * h, 2)], lev_rs.at[1, e, h])
        for a in range(VARIABLES):
            both = [recv_b[2 * a + half, e].reshape(128, 128) for half in range(2)]
            out = jnp.zeros((128, 256), F32)
            for b in range(COV_BANDS):
                x = jnp.concatenate([part * mask[b] for part in both], axis=1)
                out = out + dot(x, mix[b * VARIABLES + a])
            for p in range(2):
                rows[pl.ds(1024 * e + 2 * a + p, 128, stride=8), :] = out[:, p * 128 : p * 128 + 128]
        grad[pl.ds(1024 * e, 1024), :] = rows[pl.ds(1024 * e, 1024), :].astype(BF16)

    for h in range(2):
        legendre_back(0, h)
    for h in range(2):
        legendre_back(1, h)
    vertical_back(0)
    vertical_back(1)

    for h in range(2):
        arrived(leg.at[pl.ds(2 * h, 2), pl.ds(0, 7)], leg_ss.at[h])
        for e in range(2):
            for d in range(2):
                arrived(recv_f.at[e, pl.ds(2 * h, 2), pl.ds(0, 7)], lev_ss.at[d, e, h])
                arrived(c1.at[e, h, pl.ds(0, 63)], wave_ss.at[d, e, h])


def deliver(inc, grad, inc_h, grad_h, sem):
    copies = (
        pltpu.make_async_copy(inc, inc_h, sem.at[0]),
        pltpu.make_async_copy(grad, grad_h, sem.at[1]),
    )
    for copy in copies:
        copy.start()
    for copy in copies:
        copy.wait()


def shards(control, wave_of_slot, legendre, vertical, points, lat_band, grid_scale, obs_weight):
    members, slots, rows_dev = control.shape[0], control.shape[1], control.shape[2]
    count = members * slots * rows_dev
    flat = control.reshape(count, 2, 4, 128).transpose(0, 2, 1, 3).reshape(count * 8, 128)
    vmem = pl.BlockSpec(memory_space=pltpu.VMEM)
    hbm = pl.BlockSpec(memory_space=pltpu.HBM)
    wide = (2, 2, 64, 8, 128)
    increment, gradient = pl.pallas_call(
        kernel,
        out_shape=(
            jax.ShapeDtypeStruct((2, 4, 64, 512), BF16),
            jax.ShapeDtypeStruct((2048, 128), BF16),
        ),
        in_specs=[hbm] * 8,
        out_specs=(vmem, vmem),
        scratch_shapes=[
            pltpu.VMEM((2, 128), jnp.int32),
            pltpu.VMEM((1, 4), jnp.int32),
            pltpu.VMEM((1, 4), jnp.int32),
            pltpu.VMEM((2048, 128), BF16),
            pltpu.VMEM((4, 32, 256), BF16),
            pltpu.VMEM((16, 128, 128), BF16),
            pltpu.VMEM((8, 64), F32),
            pltpu.VMEM((4, 64, 512), BF16),
            pltpu.VMEM((2048, 128), F32),
            pltpu.VMEM((4, 128, 128), BF16),
            pltpu.VMEM((16, 256, 256), BF16),
            pltpu.VMEM((8, 2, 4, 32, 128), BF16),
            pltpu.VMEM((2, 4, 8, 32, 128), BF16),
            pltpu.VMEM((4, 8, 32, 256), BF16),
            pltpu.VMEM((4, 256, 256), BF16),
            pltpu.VMEM((256, 128), F32),
            pltpu.VMEM((4, 2, 2, 128, 512), BF16),
            pltpu.VMEM(wide, BF16),
            pltpu.VMEM(wide, BF16),
            pltpu.VMEM((4, 64, 512), F32),
            pltpu.VMEM((4, 128, 512), BF16),
            pltpu.VMEM((2, 512, 128), F32),
            pltpu.VMEM(wide, BF16),
            pltpu.VMEM(wide, BF16),
            pltpu.VMEM((8, 2, 4, 32, 128), BF16),
            pltpu.VMEM((8, 2, 4, 32, 128), BF16),
            pltpu.SemaphoreType.DMA((8,)),
            pltpu.SemaphoreType.REGULAR,
            pltpu.SemaphoreType.REGULAR,
            pltpu.SemaphoreType.DMA((2,)),
            pltpu.SemaphoreType.DMA((2,)),
            pltpu.SemaphoreType.DMA((2,)),
            pltpu.SemaphoreType.DMA((2, 2, 2)),
            pltpu.SemaphoreType.DMA((2, 2, 2)),
            pltpu.SemaphoreType.DMA((2, 2, 2)),
            pltpu.SemaphoreType.DMA((2, 2, 2)),
        ],
        compiler_params=pltpu.CompilerParams(
            collective_id=0, has_side_effects=True, vmem_limit_bytes=24_000_000
        ),
    )(
        *(
            pltpu.with_memory_space_constraint(x, pltpu.HBM)
            for x in (
                wave_of_slot.reshape(2, 128), points.reshape(1, 4), lat_band.reshape(1, 4), flat,
                legendre, vertical.reshape(16, 128, 128), grid_scale, obs_weight,
            )
        )
    )
    increment, gradient = pl.pallas_call(
        deliver,
        out_shape=(
            jax.ShapeDtypeStruct((2, 4, 64, 512), BF16),
            jax.ShapeDtypeStruct((2048, 128), BF16),
        ),
        in_specs=[vmem, vmem],
        out_specs=(hbm, hbm),
        scratch_shapes=[pltpu.SemaphoreType.DMA((2,))],
        compiler_params=pltpu.CompilerParams(vmem_limit_bytes=24_000_000),
    )(increment, gradient)
    gradient = gradient.reshape(count, 4, 2, 128).transpose(0, 2, 1, 3)
    return increment, gradient.reshape(control.shape)


def solution(mesh):
    in_specs = (
        P(None, "wave", "lev", None, None),
        P(),
        P("wave", "lev", None),
        P(),
        P("wave"),
        P("wave"),
        P(None, "lev"),
        P("wave", "lev", None),
    )
    out_specs = (P(None, "wave", "lev", None), P(None, "wave", "lev", None, None))
    return jax.shard_map(shards, mesh=mesh, in_specs=in_specs, out_specs=out_specs, check_vma=False)
```
